32 devices in a mesh: dp: 8 (over y, x, core), tensor: 4 (over z).
Axes of the slice: x: 2, y: 2, z: 4, core: 2. Of those that a mesh axis runs over, the one named last changes fastest.
Arguments:
- saved_input: bfloat16 [2048, 6144], P('dp', 'tensor'), may hold values from -6 to 6
- queries: bfloat16 [2048, 1024], P('dp', 'tensor'), may hold values from -8 to 8
- keys: bfloat16 [2048, 1024], P('dp', 'tensor'), may hold values from -8 to 8
- value_weight: bfloat16 [6144, 1024], P(None, 'tensor'), may hold values from -0.109375 to 0.109375
- grad_attended: bfloat16 [2048, 1024], P('dp', 'tensor'), may hold values from -6 to 6
Outputs:
- grad_input: bfloat16 [2048, 6144], P('dp', 'tensor')
- grad_value_weight: float32 [6144, 1024], P('dp', 'tensor')
- grad_queries: bfloat16 [2048, 1024], P('dp', 'tensor')
- grad_keys: bfloat16 [2048, 1024], P('dp', 'tensor')
The draws below stay inside these ranges and needn't reach their ends.
All inputs are finite; a program needn't handle non-finite values.
Results may differ from the reference program's by a relative error of at most 0.02.
Values may be sent and summed in bfloat16 or wider, within the bound.
A program may use at most 64 MiB of HBM per device.

```python
import jax
import jax.numpy as jnp
from jax import lax

D = 6144
HD = 128
HEADS_DEV = 2
SEQ = 256
HEADS = 8
GROUPS = 8
TOKENS = 2048


def paired_fields(key):
    query_seed, key_seed = jax.random.split(jax.random.fold_in(key, 7919))
    field_shape = (TOKENS, HEADS, HD)
    query_field = jax.random.truncated_normal(query_seed, -5.0, 5.0, field_shape, jnp.float32)
    key_field = jax.random.truncated_normal(key_seed, -5.0, 5.0, field_shape, jnp.float32)
    total_width = HEADS * HD
    return (query_field.reshape(TOKENS, total_width).astype(jnp.bfloat16), key_field.reshape(TOKENS, total_width).astype(jnp.bfloat16))


def draw_queries(key, part):
    return paired_fields(key)[0]


def draw_keys(key, part):
    return paired_fields(key)[1]


def strengthened(drawn, rng, source, target, parts, factor):
    owner, partner = [(jnp.arange(drawn.shape[dim]) // (drawn.shape[dim] // parts)).reshape([-1 if axis == dim else 1 for axis in range(drawn.ndim)]) for dim in (source, target)]
    chosen = jax.random.permutation(rng, parts)[partner]
    strong = (owner == chosen) | (owner == (partner + parts // 2) % parts)
    return jnp.where(strong, factor * drawn, drawn)


def block_levels(key, dims, cuts, low, largest):
    factor_of, own = 1.0, jax.random.fold_in(key, 6)
    for axis_at, blocks in cuts:
        steps = jnp.exp(jax.random.uniform(jax.random.fold_in(own, axis_at), (blocks,), jnp.float32, low / len(cuts), largest / len(cuts)))
        factor_of = factor_of * jnp.repeat(steps, dims[axis_at] // blocks).reshape([-1 if axis == axis_at else 1 for axis in range(len(dims))])
    return factor_of


def bell_draw(key, shape, width, reach, shards=(), kind=jnp.bfloat16):
    loudness = block_levels(key, shape, shards, -0.22, 0.18) if shards else 1.0
    values = jax.random.normal(key, shape, jnp.float32) * width * loudness
    return jnp.minimum(jnp.maximum(values, -reach), reach).astype(kind)


def bell_draw_with(rng, extent, width, most, shards, heavy, kind=jnp.bfloat16):
    entries = width * jax.random.normal(rng, extent, jnp.float32)
    if shards:
        entries = entries * block_levels(rng, extent, shards, -0.22, 0.18)
    return jnp.clip(strengthened(entries, jax.random.fold_in(rng, 3), *heavy), -most, most).astype(kind)


def setup_inputs(seed: int = 0) -> dict:
    key_list = jax.random.split(jax.random.key(seed), 6)
    saved_input = bell_draw_with(key_list[0], (TOKENS, D), 1.0, 6.0, ((0, 8), (1, 4)), (0, 1, 8, 2.0))
    queries = draw_queries(jax.random.fold_in(key_list[5], 71), 0)
    keys = draw_keys(jax.random.fold_in(key_list[5], 71), 0)
    value_weight = bell_draw_with(key_list[3], (D, HEADS * HD), D ** -0.5, 0.109375, ((1, 4),), (1, 0, 4, 2.0))
    grad_attended = bell_draw(key_list[4], (TOKENS, HEADS * HD), 1.0, 6.0, ((0, 8), (1, 4)))
    return dict(saved_input=saved_input, queries=queries, keys=keys, value_weight=value_weight, grad_attended=grad_attended)


def attention_backward(group_query, group_key, group_values, group_grad, causal):
    score_scale = 1.0 / jnp.sqrt(jnp.float32(HD))
    query_heads = group_query.astype(jnp.float32).reshape(SEQ, HEADS, HD)
    key_heads = group_key.astype(jnp.float32).reshape(SEQ, HEADS, HD)
    value_heads = group_values.astype(jnp.float32).reshape(SEQ, HEADS, HD)
    grad_heads = group_grad.astype(jnp.float32).reshape(SEQ, HEADS, HD)
    scores = jnp.einsum('qhd,khd->hqk', query_heads, key_heads) * score_scale
    scores = jnp.where(causal[None], scores, -jnp.inf)
    row_max = lax.optimization_barrier(jnp.max(scores, axis=-1, keepdims=True))
    weights_exp = jnp.exp(scores - row_max)
    attention = weights_exp / lax.optimization_barrier(jnp.sum(weights_exp, axis=-1, keepdims=True))
    probs_half = attention.astype(jnp.bfloat16).astype(jnp.float32)
    grad_values = jnp.einsum('hqk,qhd->khd', probs_half, grad_heads).astype(jnp.bfloat16)
    grad_probs = jnp.einsum('qhd,khd->hqk', grad_heads, value_heads)
    row_dot = lax.optimization_barrier(jnp.sum(attention * grad_probs, axis=-1, keepdims=True))
    grad_scores = (attention * (grad_probs - row_dot) * score_scale).astype(jnp.bfloat16).astype(jnp.float32)
    grad_queries = jnp.einsum('hqk,khd->qhd', grad_scores, key_heads).astype(jnp.bfloat16)
    grad_keys = jnp.einsum('hqk,qhd->khd', grad_scores, query_heads).astype(jnp.bfloat16)
    total_width = HEADS * HD
    return (grad_values.reshape(SEQ, total_width), grad_queries.reshape(SEQ, total_width), grad_keys.reshape(SEQ, total_width))

def reference(saved_input, queries, keys, value_weight, grad_attended):
    total_width = HEADS * HD
    block_width = HEADS_DEV * HD
    block_count = total_width // block_width
    weight_blocks = value_weight.astype(jnp.float32).reshape(D, block_count, block_width)
    positions = jnp.arange(SEQ)
    causal = positions[:, None] >= positions[None, :]

    def one_group(total, inputs):
        group_input, group_query, group_key, group_grad = inputs
        values = jnp.dot(group_input, value_weight, preferred_element_type=jnp.float32).astype(jnp.bfloat16)
        grad_values, grad_queries, grad_keys = attention_backward(group_query, group_key, values, group_grad, causal)
        value_blocks = grad_values.astype(jnp.float32).reshape(SEQ, block_count, block_width)
        partial_value = jnp.einsum('tnc,dnc->ntd', value_blocks, weight_blocks)
        partial_value = lax.optimization_barrier(partial_value.astype(jnp.bfloat16)).astype(jnp.float32)
        grad_input = lax.optimization_barrier(jnp.sum(partial_value, axis=0)).astype(jnp.bfloat16)
        weight_term = jnp.dot(group_input.T, grad_values, preferred_element_type=jnp.float32)
        weight_term = lax.optimization_barrier(weight_term.astype(jnp.bfloat16)).astype(jnp.float32)
        return (total + weight_term, (grad_input, grad_queries, grad_keys))
    stacked = (saved_input.reshape(GROUPS, SEQ, D), queries.reshape(GROUPS, SEQ, total_width), keys.reshape(GROUPS, SEQ, total_width), grad_attended.reshape(GROUPS, SEQ, total_width))
    total, results = lax.scan(one_group, jnp.zeros((D, total_width), jnp.float32), stacked)
    grad_input, grad_queries, grad_keys = results
    grad_value_weight = total / jnp.float32(GROUPS)
    return (grad_input.reshape(TOKENS, D), grad_value_weight, grad_queries.reshape(TOKENS, total_width), grad_keys.reshape(TOKENS, total_width))
```

```python
import functools
import math

import jax
import jax.numpy as jnp
from jax import lax
from jax.experimental import pallas as pl
from jax.experimental.pallas import tpu as pltpu
from jax.sharding import PartitionSpec as P

HD = 128


def fused_kernel(
    n, chips,
    x_hbm, q_hbm, k_hbm, w, ga_hbm,
    gi, gw, gq, gk,
    x, queries, keys, ga,
    wfull, gvall, xt, qs, r1x, r1y, t2, r2x, r2y, zs, fin,
    part, vsend, vrecv, vals, probs, wsend,
    send_sem, recv_sem, load_sem,
):
    f32, bf16 = jnp.float32, jnp.bfloat16
    tokens, width = queries.shape
    feat = x.shape[1]
    crows = feat // chips
    hr = crows // 2
    heads = width // HD
    t = lax.axis_index("tensor")
    d = lax.axis_index("dp")
    c, k = d // 2, d % 2
    cx, cy = c % 2, c // 2
    scale = 1.0 / (HD ** 0.5)
    last = n - 1
    upper = t // (n // 2)
    edge = (t % last) == 0
    mid = (t % last) != 0
    outer = jnp.where(edge, 1, 0)
    level = [t, t + 1 - 2 * (t % 2), last - last * upper, n // 2 - upper]

    def at(s):
        return (d, s)

    partner = (d + 1 - 2 * k, t)
    xn = (d + 2 - 4 * cx, t)
    yn = (d + 4 - 8 * cy, t)
    diagonal = (d + 2 - 4 * cx + 4 - 8 * cy, t)
    chip_x, chip_y, chip_d = c + 1 - 2 * cx, c + 2 - 4 * cy, last - c

    counts = [0, 0]
    pending = []

    def slot():
        counts[1] += 1
        return counts[1] - 1

    def slots():
        return [slot() for _ in range(n)]

    def copy(src, dst, device, recv, when=None):
        i = counts[0]
        counts[0] += 1
        cp = pltpu.make_async_remote_copy(
            src_ref=src, dst_ref=dst, send_sem=send_sem.at[i], recv_sem=recv_sem.at[recv],
            device_id=device, device_id_type=pl.DeviceIdType.MESH,
        )
        if when is None:
            cp.start()
        else:
            pl.when(when)(cp.start)
        pending.append((i, math.prod(src.shape) // width, when))

    def drain(sent):
        for i, size, when in sent:
            ref = wfull.at[0, 0:size]
            cp = pltpu.make_async_remote_copy(
                src_ref=ref, dst_ref=ref, send_sem=send_sem.at[i], recv_sem=recv_sem.at[0],
                device_id=partner, device_id_type=pl.DeviceIdType.MESH,
            )
            if when is None:
                cp.wait_send()
            else:
                pl.when(when)(cp.wait_send)

    def arrive(recv, ref):
        pltpu.make_async_remote_copy(
            src_ref=ref, dst_ref=ref, send_sem=send_sem.at[0], recv_sem=recv_sem.at[recv],
            device_id=partner, device_id_type=pl.DeviceIdType.MESH,
        ).wait_recv()

    def rows(i, size):
        return pl.ds(pl.multiple_of(i * size, size), size)

    mine, theirs = rows(k, tokens), rows(1 - k, tokens)

    barrier = pltpu.get_barrier_semaphore()
    peers = [at((t + o) % n) for o in range(1, n)] + [xn, yn, diagonal, partner]
    for peer in peers:
        pl.semaphore_signal(
            barrier, inc=1, device_id=peer, device_id_type=pl.DeviceIdType.MESH
        )
    loads = [
        pltpu.make_async_copy(src, dst, load_sem.at[i])
        for i, (src, dst) in enumerate([
            (q_hbm, queries), (k_hbm, keys), (ga_hbm, ga), (x_hbm, x.at[mine]),
            (w.at[rows(t, feat)], wfull.at[t]),
        ])
    ]
    for load in loads:
        load.start()
    ahead = [
        pltpu.make_async_copy(
            w.at[pl.ds(pl.multiple_of(level[i] * feat + c * crows, crows), crows)],
            wsend.at[i - 1], load_sem.at[4 + i],
        )
        for i in range(1, n)
    ]
    for load in ahead:
        load.start()
    for load in loads[:3]:
        load.wait()

    row = lax.broadcasted_iota(jnp.int32, (tokens, tokens), 0)
    col = lax.broadcasted_iota(jnp.int32, (tokens, tokens), 1)
    causal = row >= col
    for h in range(heads):
        cols = slice(h * HD, (h + 1) * HD)
        scores = lax.dot_general(
            queries[:, cols], keys[:, cols], (((1,), (1,)), ((), ())),
            preferred_element_type=f32,
        ) * scale
        scores = jnp.where(causal, scores, -jnp.inf)
        e = jnp.exp(scores - jnp.max(scores, axis=-1, keepdims=True))
        p = e / jnp.sum(e, axis=-1, keepdims=True)
        probs[h] = p
        gvall[t, mine, cols] = lax.dot_general(
            p.astype(bf16), ga[:, cols], (((0,), (0,)), ((), ())),
            preferred_element_type=f32,
        ).astype(bf16)
    for load in ahead:
        load.wait()
    loads[3].wait()
    pl.semaphore_wait(barrier, len(peers))

    xs, gvs, ws, vs = slot(), slots(), slots(), slot()
    gza, gzb = slots(), slots()
    wz, wpx, wpy, wqx, wqy, wrx, wry = (slots() for _ in range(7))
    p1x, p1y, p2x, p2y = slots(), slots(), slots(), slots()
    vz = slots()
    fs = [slot() for _ in range(chips // 2)]
    home = c == t
    here = jnp.logical_and(home, cy == 1)
    away = jnp.logical_not(here)
    contract = (((1,), (1,)), ((), ()))

    def grad_in():
        acc = lax.dot_general(
            gvall[t, mine, :], wfull[t], contract, preferred_element_type=f32
        )
        for i in range(1, n):
            acc = acc + lax.dot_general(
                gvall[level[i], mine, :], wfull[level[i]], contract,
                preferred_element_type=f32,
            )
        gi[...] = acc.astype(bf16)

    @pl.when(k == 0)
    def _():
        def chunk(i, who, first=0, size=crows):
            start = pl.multiple_of(who * crows, crows) + first
            return wfull.at[level[i], pl.ds(pl.multiple_of(start, hr), size)]

        for i in (2, 3, 1):
            copy(
                wsend.at[i - 1],
                wfull.at[t, rows(c, crows)],
                at(level[i]),
                wz[1] if i == 1 else wz[3] - outer,
            )
        copy(gvall.at[t, mine], gvall.at[t, mine], partner, gvs[0])
        copy(x.at[mine], x.at[mine], partner, xs)

        def spread(i):
            arrive(wz[i], chunk(i, c))
            low, high = chunk(i, c, 0, hr), chunk(i, c, hr, hr)
            copy(high, high, xn, wpx[i])
            copy(low, low, yn, wpy[i])
            copy(low, low, xn, wqx[i])
            copy(high, high, yn, wqy[i])

        def spread_on(i):
            piece = chunk(i, chip_x, hr, hr)
            arrive(wpx[i], piece)
            copy(piece, piece, yn, wry[i])
            piece = chunk(i, chip_y, 0, hr)
            arrive(wpy[i], piece)
            copy(piece, piece, xn, wrx[i])

        def spread_end(i):
            arrive(wqx[i], chunk(i, chip_x, 0, hr))
            arrive(wqy[i], chunk(i, chip_y, hr, hr))
            arrive(wrx[i], chunk(i, chip_d, 0, hr))
            arrive(wry[i], chunk(i, chip_d, hr, hr))
            copy(wfull.at[level[i]], wfull.at[level[i]], partner, ws[i])

        def value_part(i):
            part[i - 1] = jnp.dot(x[...], wfull[level[i]], preferred_element_type=f32)
            if i == 1:
                vsend[0] = part[0].astype(bf16)
                copy(vsend.at[0], vrecv.at[1], at(level[1]), vz[1])
            else:
                @pl.when(edge)
                def _():
                    vsend[i - 1] = part[i - 1].astype(bf16)
                copy(vsend.at[i - 1], vrecv.at[i], at(level[1]), vz[i], when=edge)

        def value_sum(i):
            @pl.when(mid)
            def _():
                arrive(vz[i], vrecv.at[i])
                vsend[i - 1] = (part[i - 1] + vrecv[i].astype(f32)).astype(bf16)
            copy(vsend.at[i - 1], vrecv.at[0], at(level[i]), vz[0], when=mid)

        spread(2)
        spread(1)
        spread_on(2)
        spread(3)
        spread_on(1)
        arrive(xs, x.at[theirs])
        spread_on(3)
        spread_end(2)
        value_part(2)
        spread_end(3)
        value_part(3)
        spread_end(1)
        value_part(1)
        value_sum(2)
        value_sum(3)
        loads[4].wait()
        part[0] = jnp.dot(x[...], wfull[t], preferred_element_type=f32)
        for i in range(1, n):
            arrive(gvs[i], gvall.at[level[i], mine])
        grad_in()
        arrive(vz[1], vrecv.at[1])
        arrive(vz[0], vrecv.at[0])
        vals[...] = (
            part[0] + vrecv[1].astype(f32) + vrecv[0].astype(f32)
        ).astype(bf16)
        copy(vals.at[theirs], vals.at[theirs], partner, vs)

    sent_w = list(pending)
    pending.clear()

    @pl.when(k == 1)
    def _():
        def gv(i, which):
            return gvall.at[level[i], which]

        def send_gv():
            for to, far in ((1, 0), (3, outer)):
                for which, got in ((mine, gza), (theirs, gzb)):
                    copy(gv(0, which), gv(0, which), at(level[to]), got[to] - far)

        copy(x.at[mine], x.at[mine], partner, xs)
        arrive(gvs[0], gv(0, theirs))

        def pass_on(i):
            @pl.when(mid)
            def _():
                arrive(gza[i], gv(i, mine))
            copy(gv(i, mine), gv(i, mine), at(level[1]), gza[i], when=mid)

            @pl.when(mid)
            def _():
                arrive(gzb[i], gv(i, theirs))
            copy(gv(i, theirs), gv(i, theirs), at(level[1]), gzb[i], when=mid)

        def pass_over(i):
            @pl.when(edge if i > 1 else t >= 0)
            def _():
                arrive(gza[i], gv(i, mine))
                arrive(gzb[i], gv(i, theirs))
            copy(gv(i, theirs), gv(i, theirs), partner, gvs[i])

        def weight_term(i):
            term = jnp.dot(xt[...], gvall[level[i]], preferred_element_type=f32).astype(bf16)
            for j in range(chips):
                qs[i, j // 2, j % 2] = term[j * crows:(j + 1) * crows]
            copy(qs.at[i, :, 1 - cx, 0:hr, :], r1x.at[i], xn, p1x[i])
            copy(qs.at[i, 1 - cy, :, hr:crows, :], r1y.at[i], yn, p1y[i])

        def second_phase(i):
            arrive(p1x[i], r1x.at[i])
            t2[i, 0] = (
                qs[i, 1 - cy, cx, 0:hr, :].astype(f32) + r1x[i, 1 - cy].astype(f32)
            ).astype(bf16)
            copy(t2.at[i, 0], r2y.at[i], yn, p2y[i])
            arrive(p1y[i], r1y.at[i])
            t2[i, 1] = (
                qs[i, cy, 1 - cx, hr:crows, :].astype(f32) + r1y[i, 1 - cx].astype(f32)
            ).astype(bf16)
            copy(t2.at[i, 1], r2x.at[i], xn, p2x[i])

        def finish(i):
            arrive(p2y[i], r2y.at[i])
            zs[i, 0:hr, :] = (
                qs[i, cy, cx, 0:hr, :].astype(f32) + r1x[i, cy].astype(f32)
                + r2y[i].astype(f32)
            ).astype(bf16)
            arrive(p2x[i], r2x.at[i])
            zs[i, hr:crows, :] = (
                qs[i, cy, cx, hr:crows, :].astype(f32) + r1y[i, cx].astype(f32)
                + r2x[i].astype(f32)
            ).astype(bf16)
            if i == 0:
                @pl.when(here)
                def _():
                    fin[cx] = zs[0]
            copy(
                zs.at[i], fin.at[cx], (2 * t + cy, level[i]), fs[0] + cx,
                when=away if i == 0 else None,
            )

        xt[:, mine] = x[mine, :].T
        arrive(xs, x.at[theirs])
        xt[:, theirs] = x[theirs, :].T
        weight_term(0)
        second_phase(0)
        send_gv()
        pass_on(3)
        pass_over(1)
        weight_term(1)
        pass_on(2)
        pass_over(3)
        weight_term(3)
        second_phase(1)
        pass_over(2)
        weight_term(2)
        second_phase(3)
        finish(1)
        second_phase(2)
        finish(3)
        finish(2)
        finish(0)
        loads[4].wait()
        for i in range(1, n):
            arrive(ws[i], wfull.at[level[i]])
        grad_in()
        arrive(vs, vals.at[mine])

    sent_g = list(pending)
    pending.clear()

    for h in range(heads):
        cols = slice(h * HD, (h + 1) * HD)
        grad_probs = lax.dot_general(
            ga[:, cols], vals[mine, cols], contract, preferred_element_type=f32
        )
        p = probs[h]
        row_dot = jnp.sum(p * grad_probs, axis=-1, keepdims=True)
        gs = (p * (grad_probs - row_dot) * scale).astype(bf16)
        gq[:, cols] = jnp.dot(gs, keys[:, cols], preferred_element_type=f32).astype(bf16)
        gk[:, cols] = lax.dot_general(
            gs, queries[:, cols], (((0,), (0,)), ((), ())), preferred_element_type=f32
        ).astype(bf16)

    groups = float(2 * chips)
    for j in range(chips // 2):
        local = jnp.logical_and(here, jnp.logical_and(k == 1, cx == j))

        @pl.when(jnp.logical_not(local))
        def _():
            arrive(fs[j], fin.at[j])
        gw[j * crows:(j + 1) * crows, :] = fin[j].astype(f32) / groups

    for role, sent in enumerate((sent_w, sent_g)):
        @pl.when(k == role)
        def _():
            drain(sent)
    assert counts[0] <= send_sem.shape[0] and counts[1] <= recv_sem.shape[0], counts


def write_out(*refs):
    results, outs, sem = refs[:4], refs[4:8], refs[8]
    moves = [
        pltpu.make_async_copy(results[i], outs[i], sem.at[i]) for i in range(4)
    ]
    for move in moves:
        move.start()
    for move in moves:
        move.wait()


def fused(n, groups, saved_input, queries, keys, value_weight, grad_attended):
    chips = groups // 2
    tokens, feat = saved_input.shape
    depth, width = value_weight.shape
    crows = feat // chips
    bf16 = jnp.bfloat16
    levels = n - 1
    vmem = pl.BlockSpec(memory_space=pltpu.VMEM)
    results = pl.pallas_call(
        functools.partial(fused_kernel, n, chips),
        out_shape=(
            pltpu.VMEM((tokens, feat), bf16),
            pltpu.VMEM((depth // groups, width), jnp.float32),
            pltpu.VMEM(queries.shape, bf16),
            pltpu.VMEM(keys.shape, bf16),
        ),
        in_specs=[pl.BlockSpec(memory_space=pl.ANY)] * 5,
        out_specs=(vmem,) * 4,
        scratch_shapes=[
            pltpu.VMEM((2 * tokens, feat), bf16),
            pltpu.VMEM(queries.shape, bf16),
            pltpu.VMEM(keys.shape, bf16),
            pltpu.VMEM(grad_attended.shape, bf16),
            pltpu.VMEM((n, feat, width), bf16),
            pltpu.VMEM((n, 2 * tokens, width), bf16),
            pltpu.VMEM((feat, 2 * tokens), bf16),
            pltpu.VMEM((n, 2, chips // 2, crows, width), bf16),
            pltpu.VMEM((n, 2, crows // 2, width), bf16),
            pltpu.VMEM((n, 2, crows // 2, width), bf16),
            pltpu.VMEM((n, 2, crows // 2, width), bf16),
            pltpu.VMEM((n, crows // 2, width), bf16),
            pltpu.VMEM((n, crows // 2, width), bf16),
            pltpu.VMEM((n, crows, width), bf16),
            pltpu.VMEM((chips // 2, crows, width), bf16),
            pltpu.VMEM((levels, 2 * tokens, width), jnp.float32),
            pltpu.VMEM((levels, 2 * tokens, width), bf16),
            pltpu.VMEM((n, 2 * tokens, width), bf16),
            pltpu.VMEM((2 * tokens, width), bf16),
            pltpu.VMEM((width // HD, tokens, tokens), jnp.float32),
            pltpu.VMEM((levels, crows, width), bf16),
            pltpu.SemaphoreType.DMA((96,)),
            pltpu.SemaphoreType.DMA((96,)),
            pltpu.SemaphoreType.DMA((8,)),
        ],
        compiler_params=pltpu.CompilerParams(
            collective_id=0, has_side_effects=True, vmem_limit_bytes=58 * 2**20
        ),
    )(saved_input, queries, keys, value_weight, grad_attended)
    return pl.pallas_call(
        write_out,
        out_shape=tuple(jax.ShapeDtypeStruct(r.shape, r.dtype) for r in results),
        in_specs=[vmem] * 4,
        out_specs=(pl.BlockSpec(memory_space=pl.ANY),) * 4,
        scratch_shapes=[pltpu.SemaphoreType.DMA((4,))],
        compiler_params=pltpu.CompilerParams(vmem_limit_bytes=8 * 2**20),
    )(*results)


def on_device(saved_input, queries, keys, value_weight, grad_attended):
    token_count = queries.shape[0]
    local_width = value_weight.shape[1]
    local_heads = local_width // HD
    score_scale = 1.0 / jnp.sqrt(jnp.float32(HD))
    full_input = lax.all_gather(saved_input, "tensor", axis=1, tiled=True)
    values = jnp.dot(full_input, value_weight, preferred_element_type=jnp.float32).astype(
        jnp.bfloat16
    )
    query_heads = queries.reshape(token_count, local_heads, HD)
    key_heads = keys.reshape(token_count, local_heads, HD)
    value_heads = values.reshape(token_count, local_heads, HD)
    grad_heads = grad_attended.reshape(token_count, local_heads, HD)
    scores = (
        jnp.einsum("qhd,khd->hqk", query_heads, key_heads, preferred_element_type=jnp.float32)
        * score_scale
    )
    positions = lax.iota(jnp.int32, token_count)
    causal = positions[:, None] >= positions[None, :]
    scores = jnp.where(causal[None], scores, -jnp.inf)
    row_max = jnp.max(scores, axis=-1, keepdims=True)
    weights_exp = jnp.exp(scores - row_max)
    attention = weights_exp / jnp.sum(weights_exp, axis=-1, keepdims=True)
    probs_half = attention.astype(jnp.bfloat16)
    grad_values = jnp.einsum(
        "hqk,qhd->khd", probs_half, grad_heads, preferred_element_type=jnp.float32
    ).astype(jnp.bfloat16)
    grad_probs = jnp.einsum(
        "qhd,khd->hqk", grad_heads, value_heads, preferred_element_type=jnp.float32
    )
    row_dot = jnp.sum(attention * grad_probs, axis=-1, keepdims=True)
    grad_scores = (attention * (grad_probs - row_dot) * score_scale).astype(jnp.bfloat16)
    grad_queries = jnp.einsum(
        "hqk,khd->qhd", grad_scores, key_heads, preferred_element_type=jnp.float32
    ).astype(jnp.bfloat16)
    grad_keys = jnp.einsum(
        "hqk,qhd->khd", grad_scores, query_heads, preferred_element_type=jnp.float32
    ).astype(jnp.bfloat16)
    value_flat = grad_values.reshape(token_count, local_width)
    data_groups = lax.axis_size("dp")
    partial_value = lax.dot_general(
        value_flat, value_weight, (((1,), (1,)), ((), ())), preferred_element_type=jnp.float32
    )
    grad_input = lax.psum_scatter(
        partial_value.astype(jnp.bfloat16), "tensor", scatter_dimension=1, tiled=True
    )
    partial_value = lax.dot_general(
        full_input, value_flat, (((0,), (0,)), ((), ())), preferred_element_type=jnp.float32
    )
    summed = lax.psum_scatter(
        partial_value.astype(jnp.bfloat16), "dp", scatter_dimension=0, tiled=True
    ).astype(jnp.float32)
    grad_value_weight = summed / jnp.float32(data_groups)
    return (
        grad_input,
        grad_value_weight,
        grad_queries.reshape(token_count, local_width),
        grad_keys.reshape(token_count, local_width),
    )


def solution(mesh):
    placed = (
        P("dp", "tensor"),
        P("dp", "tensor"),
        P("dp", "tensor"),
        P(None, "tensor"),
        P("dp", "tensor"),
    )
    levels, groups = mesh.shape["tensor"], mesh.shape["dp"]
    run = on_device
    if groups == 2 * levels and levels == 4:
        run = functools.partial(fused, levels, groups)
    return jax.shard_map(
        run,
        mesh=mesh,
        in_specs=placed,
        out_specs=(P("dp", "tensor"), P("dp", "tensor"), P("dp", "tensor"), P("dp", "tensor")),
        check_vma=False,
    )
```

```python
import functools
import math

import jax
import jax.numpy as jnp
from jax import lax
from jax.experimental import pallas as pl
from jax.experimental.pallas import tpu as pltpu
from jax.sharding import PartitionSpec as P

HD = 128
END_WEIGHT = (
    ("W", 2), ("W", 3), ("W", 1), ("start", 0), ("sp", 2), ("sp", 1), ("on", 2), ("x", 0),
    ("sp", 3), ("end", 2), ("on", 3), ("vp", 2), ("end", 3), ("vp", 3), ("on", 1),
    ("end", 1), ("vp", 1), ("fin", 0),
)
MIDDLE_WEIGHT = (
    ("W", 1), ("W", 3), ("start", 0), ("W", 2), ("sp", 2), ("sp", 3), ("on", 2), ("sp", 1),
    ("on", 3), ("end", 2), ("on", 1), ("x", 0), ("end", 1), ("vp", 2), ("end", 3),
    ("vp", 1), ("vp", 3), ("cs", 3), ("fin", 0),
)
END_GRAD = (
    ("tk", 1), ("start", 0), ("twin", 0), ("x", 0), ("wt", 0), ("gvm", 0), ("gvt", 0),
    ("tk", 2), ("s2", 0), ("wt", 2), ("wt", 1), ("s2", 2), ("tk", 3), ("wt", 3), ("f", 2),
    ("s2", 1), ("s2", 3), ("f", 0), ("f", 3), ("f", 1), ("fin", 0),
)
MIDDLE_GRAD = (
    ("gvm", 0), ("start", 0), ("twin", 0), ("gvt", 0), ("x", 0), ("wt", 0), ("tk", 1),
    ("tk", 3), ("wt", 3), ("wt", 1), ("tk", 2), ("s2", 3), ("wt", 2), ("s2", 1), ("f", 3),
    ("s2", 0), ("s2", 2), ("f", 2), ("f", 0), ("f", 1), ("fin", 0),
)
JOINED = (3,)


def fused_kernel(
    n, chips,
    x_hbm, q_hbm, k_hbm, w, ga_hbm,
    gi, fin, gq, gk,
    x, queries, keys, ga,
    wfull, gvall, xt, qs, r1x, r1y, t2, r2x, r2y, zs,
    part, vsend, vrecv, vsum, probs, wsend,
    send_sem, recv_sem, load_sem,
):
    f32, bf16 = jnp.float32, jnp.bfloat16
    tokens, width = queries.shape
    feat = x.shape[1]
    crows = feat // chips
    hr = crows // 2
    heads = width // HD
    t = lax.axis_index("tensor")
    d = lax.axis_index("dp")
    c, k = d // 2, d % 2
    cx, cy = c % 2, c // 2
    scale = 1.0 / (HD ** 0.5)
    last = n - 1
    upper = t // (n // 2)
    edge = (t % last) == 0
    mid = (t % last) != 0
    level = [t, t + 1 - 2 * (t % 2), last - last * upper, n // 2 - upper]

    def at(s):
        return (d, s)

    partner = (d + 1 - 2 * k, t)
    xn = (d + 2 - 4 * cx, t)
    yn = (d + 4 - 8 * cy, t)
    diagonal = (d + 2 - 4 * cx + 4 - 8 * cy, t)
    chip_x, chip_y, chip_d = c + 1 - 2 * cx, c + 2 - 4 * cy, last - c

    counts = [0, 0]
    sent = {}
    now = [None]

    def slot():
        counts[1] += 1
        return counts[1] - 1

    def slots():
        return [slot() for _ in range(n)]

    def copy(src, dst, device, recv):
        i = counts[0]
        counts[0] += 1
        cp = pltpu.make_async_remote_copy(
            src_ref=src, dst_ref=dst, send_sem=send_sem.at[i], recv_sem=recv_sem.at[recv],
            device_id=device, device_id_type=pl.DeviceIdType.MESH,
        )
        cp.start()
        sent.setdefault(now[0], []).append((i, math.prod(src.shape) * src.dtype.itemsize // (2 * width)))

    def drain(name):
        for i, size in sent[name]:
            ref = wfull.at[0, 0:size]
            pltpu.make_async_remote_copy(
                src_ref=ref, dst_ref=ref, send_sem=send_sem.at[i], recv_sem=recv_sem.at[0],
                device_id=partner, device_id_type=pl.DeviceIdType.MESH,
            ).wait_send()

    def arrive(recv, ref):
        pltpu.make_async_remote_copy(
            src_ref=ref, dst_ref=ref, send_sem=send_sem.at[0], recv_sem=recv_sem.at[recv],
            device_id=partner, device_id_type=pl.DeviceIdType.MESH,
        ).wait_recv()

    def rows(i, size):
        return pl.ds(pl.multiple_of(i * size, size), size)

    mine, theirs = rows(k, tokens), rows(1 - k, tokens)

    barrier = pltpu.get_barrier_semaphore()
    peers = [at((t + o) % n) for o in range(1, n)] + [xn, yn, diagonal, partner]
    for peer in peers:
        pl.semaphore_signal(
            barrier, inc=1, device_id=peer, device_id_type=pl.DeviceIdType.MESH
        )
    ahead = [
        pltpu.make_async_copy(
            w.at[pl.ds(pl.multiple_of(level[i] * feat + c * crows, crows), crows)],
            wsend.at[i - 1], load_sem.at[4 + i],
        )
        for i in range(1, n)
    ]
    loads = [
        pltpu.make_async_copy(src, dst, load_sem.at[i])
        for i, (src, dst) in enumerate([
            (q_hbm, queries), (k_hbm, keys), (ga_hbm, ga), (x_hbm, x.at[mine]),
            (w.at[rows(t, feat)], wfull.at[t]),
        ])
    ]

    @pl.when(k == 0)
    def _():
        for load in ahead:
            load.start()
    for load in loads[:4]:
        load.start()

    def attend():
        for load in loads[:3]:
            load.wait()
        row = lax.broadcasted_iota(jnp.int32, (tokens, tokens), 0)
        col = lax.broadcasted_iota(jnp.int32, (tokens, tokens), 1)
        causal = row >= col
        for h in range(heads):
            cols = slice(h * HD, (h + 1) * HD)
            scores = lax.dot_general(
                queries[:, cols], keys[:, cols], (((1,), (1,)), ((), ())),
                preferred_element_type=f32,
            ) * scale
            scores = jnp.where(causal, scores, -jnp.inf)
            e = jnp.exp(scores - jnp.max(scores, axis=-1, keepdims=True))
            p = e / jnp.sum(e, axis=-1, keepdims=True)
            probs[h] = p
            gvall[t, mine, cols] = lax.dot_general(
                p.astype(bf16), ga[:, cols], (((0,), (0,)), ((), ())),
                preferred_element_type=f32,
            ).astype(bf16)
        loads[3].wait()
        loads[4].start()

    def everyone():
        pl.semaphore_wait(barrier, len(peers))

    xs, gvs, ws, vs = slot(), slots(), slots(), slot()
    gza, gzb = slots(), slots()
    wz, wpx, wpy, wqx, wqy, wrx, wry = (slots() for _ in range(7))
    p1x, p1y, p2x, p2y = slots(), slots(), slots(), slots()
    vz, pc = slots(), slots()
    fs = [slot() for _ in range(chips // 2)]
    home = c == t
    here = jnp.logical_and(home, cy == 1)
    away = jnp.logical_not(here)
    contract = (((1,), (1,)), ((), ()))

    def grad_in():
        acc = lax.dot_general(
            gvall[t, mine, :], wfull[t], contract, preferred_element_type=f32
        )
        for i in range(1, n):
            acc = acc + lax.dot_general(
                gvall[level[i], mine, :], wfull[level[i]], contract,
                preferred_element_type=f32,
            )
        gi[...] = acc.astype(bf16)

    def chunk(i, who, first=0, size=crows):
        start = pl.multiple_of(who * crows, crows) + first
        return wfull.at[level[i], pl.ds(pl.multiple_of(start, hr), size)]

    def weight_chain(end):
        for load in ahead:
            load.wait()
        everyone()

        def send_weight(i):
            copy(
                wsend.at[i - 1],
                wfull.at[t, rows(c, crows)],
                at(level[i]),
                wz[1] if i == 1 else wz[2] if end else wz[3],
            )

        def start(_):
            attend()
            copy(gvall.at[t, mine], gvall.at[t, mine], partner, gvs[0])
            copy(x.at[mine], x.at[mine], partner, xs)

        def spread(i):
            arrive(wz[i], chunk(i, c))
            low, high = chunk(i, c, 0, hr), chunk(i, c, hr, hr)
            copy(high, high, xn, wpx[i])
            copy(low, low, yn, wpy[i])
            copy(low, low, xn, wqx[i])
            copy(high, high, yn, wqy[i])

        def spread_on(i):
            piece = chunk(i, chip_x, hr, hr)
            arrive(wpx[i], piece)
            copy(piece, piece, yn, wry[i])
            piece = chunk(i, chip_y, 0, hr)
            arrive(wpy[i], piece)
            copy(piece, piece, xn, wrx[i])

        def spread_end(i):
            arrive(wqx[i], chunk(i, chip_x, 0, hr))
            arrive(wqy[i], chunk(i, chip_y, hr, hr))
            arrive(wrx[i], chunk(i, chip_d, 0, hr))
            arrive(wry[i], chunk(i, chip_d, hr, hr))
            copy(wfull.at[level[i]], wfull.at[level[i]], partner, ws[i])

        def value_send(i, seen):
            for j in range(2):
                copy(
                    vsend.at[i - 1, rows(j, tokens)], vrecv.at[seen - 1],
                    (2 * c + j, level[i]), vz[seen],
                )

        def value_part(i):
            vsend[i - 1] = jnp.dot(
                x[...], wfull[level[i]], preferred_element_type=f32
            ).astype(bf16)
            if i not in JOINED:
                value_send(i, 1 if i == 1 else 2 if end else 3)
            elif end:
                copy(vsend.at[i - 1], vsum.at[i - 2], at(level[1]), pc[i])

        def value_join(i):
            arrive(pc[i], vsum.at[i - 2])
            vsend[i - 1] = (vsend[i - 1].astype(f32) + vsum[i - 2].astype(f32)).astype(bf16)
            value_send(i, 3)

        def close(_):
            loads[4].wait()
            own = jnp.dot(x[...], wfull[t], preferred_element_type=f32)
            part[0] = own[0:tokens]
            part[1] = own[tokens:2 * tokens]
            copy(part.at[1], part.at[0], partner, vs)
            for i in range(1, n):
                arrive(gvs[i], gvall.at[glevel(end, i), mine])
            grad_in()
            gather(end)

        steps = {
            "W": send_weight, "start": start, "sp": spread, "on": spread_on,
            "end": spread_end, "vp": value_part, "cs": value_join, "fin": close,
            "x": lambda _: arrive(xs, x.at[theirs]),
        }
        for op, i in END_WEIGHT if end else MIDDLE_WEIGHT:
            steps[op](i)

    def gather(end):
        total = part[0]
        for i in range(1, n):
            if i != 2 or (2 if end else 3) not in JOINED:
                arrive(vz[i], vrecv.at[i - 1])
                total = total + vrecv[i - 1].astype(f32)
        part[0] = total

    def glevel(end, i):
        return level[(0, 1, 3, 2)[i] if end else (0, 3, 1, 2)[i]]

    def grad_chain(end):
        def gv(i, which):
            return gvall.at[glevel(end, i), which]

        def send_gv(which, sem):
            for to, got in ((1, 2), (3, 3)) if end else ((3, 1), (1, 1)):
                copy(gv(0, which), gv(0, which), at(level[to]), sem[got])

        attend()
        everyone()
        def start(_):
            copy(x.at[mine], x.at[mine], partner, xs)

        def turn(_):
            xt[:, mine] = x[mine, :].T
            arrive(xs, x.at[theirs])
            xt[:, theirs] = x[theirs, :].T

        def take(i):
            for which, sem in ((mine, gza), (theirs, gzb)):
                arrive(sem[i], gv(i, which))
                if not end and i != 2:
                    copy(gv(i, which), gv(i, which), at(level[1]), sem[(2, 2, 2, 3)[i]])
            copy(gv(i, theirs), gv(i, theirs), partner, gvs[i])

        def weight_term(i):
            term = jnp.dot(
                xt[...], gvall[glevel(end, i)], preferred_element_type=f32
            ).astype(bf16)
            for j in range(chips):
                qs[i, j // 2, j % 2] = term[j * crows:(j + 1) * crows]
            copy(qs.at[i, :, 1 - cx, 0:hr, :], r1x.at[i], xn, p1x[i])
            copy(qs.at[i, 1 - cy, :, hr:crows, :], r1y.at[i], yn, p1y[i])

        def second_phase(i):
            arrive(p1x[i], r1x.at[i])
            t2[i, 0] = (
                qs[i, 1 - cy, cx, 0:hr, :].astype(f32) + r1x[i, 1 - cy].astype(f32)
            ).astype(bf16)
            copy(t2.at[i, 0], r2y.at[i], yn, p2y[i])
            arrive(p1y[i], r1y.at[i])
            t2[i, 1] = (
                qs[i, cy, 1 - cx, hr:crows, :].astype(f32) + r1y[i, 1 - cx].astype(f32)
            ).astype(bf16)
            copy(t2.at[i, 1], r2x.at[i], xn, p2x[i])

        def finish(i):
            arrive(p2y[i], r2y.at[i])
            zs[i, 0:hr, :] = (
                qs[i, cy, cx, 0:hr, :].astype(f32) + r1x[i, cy].astype(f32)
                + r2y[i].astype(f32)
            ).astype(bf16)
            arrive(p2x[i], r2x.at[i])
            zs[i, hr:crows, :] = (
                qs[i, cy, cx, hr:crows, :].astype(f32) + r1y[i, cx].astype(f32)
                + r2x[i].astype(f32)
            ).astype(bf16)
            if i > 0:
                copy(zs.at[i], fin.at[cx], (2 * t + cy, glevel(end, i)), fs[0] + cx)
            else:
                @pl.when(here)
                def _():
                    fin[cx] = zs[0]

                @pl.when(away)
                def _():
                    own_final().start()

        def close(_):
            loads[4].wait()
            for i in range(1, n):
                arrive(ws[i], wfull.at[level[i]])
            grad_in()
            arrive(vs, part.at[0])
            gather(end)

        steps = {
            "start": start, "x": turn, "tk": take, "wt": weight_term, "s2": second_phase,
            "f": finish, "fin": close,
            "twin": lambda _: arrive(gvs[0], gv(0, theirs)),
            "gvm": lambda _: send_gv(mine, gza),
            "gvt": lambda _: send_gv(theirs, gzb),
        }
        for op, i in END_GRAD if end else MIDDLE_GRAD:
            steps[op](i)

    def own_final():
        return pltpu.make_async_remote_copy(
            src_ref=zs.at[0], dst_ref=fin.at[cx],
            send_sem=send_sem.at[send_sem.shape[0] - 1], recv_sem=recv_sem.at[fs[0] + cx],
            device_id=(2 * t + cy, t), device_id_type=pl.DeviceIdType.MESH,
        )

    for role, chain in enumerate((weight_chain, grad_chain)):
        for end in (True, False):
            now[0] = (role, end)

            @pl.when(jnp.logical_and(k == role, edge if end else mid))
            def _():
                chain(end)

    values = part[0].astype(bf16)
    for h in range(heads):
        cols = slice(h * HD, (h + 1) * HD)
        grad_probs = lax.dot_general(
            ga[:, cols], values[:, cols], contract, preferred_element_type=f32
        )
        p = probs[h]
        row_dot = jnp.sum(p * grad_probs, axis=-1, keepdims=True)
        gs = (p * (grad_probs - row_dot) * scale).astype(bf16)
        gq[:, cols] = jnp.dot(gs, keys[:, cols], preferred_element_type=f32).astype(bf16)
        gk[:, cols] = lax.dot_general(
            gs, queries[:, cols], (((0,), (0,)), ((), ())), preferred_element_type=f32
        ).astype(bf16)

    for j in range(chips // 2):
        local = jnp.logical_and(here, jnp.logical_and(k == 1, cx == j))

        @pl.when(jnp.logical_not(local))
        def _():
            arrive(fs[j], fin.at[j])

    @pl.when(jnp.logical_and(k == 1, away))
    def _():
        own_final().wait_send()

    for role in range(2):
        for end in (True, False):
            @pl.when(jnp.logical_and(k == role, edge if end else mid))
            def _():
                drain((role, end))
    assert counts[0] < send_sem.shape[0] and counts[1] <= recv_sem.shape[0], counts


def write_out(groups, gi_in, fin, gq_in, gk_in, gi, gw, gq, gk, part, sem):
    crows = fin.shape[1]
    moves = []

    def move(src, dst):
        cp = pltpu.make_async_copy(src, dst, sem.at[len(moves)])
        cp.start()
        moves.append(cp)

    move(gi_in, gi)
    move(gq_in, gq)
    move(gk_in, gk)
    for j in range(fin.shape[0]):
        part[j] = fin[j].astype(jnp.float32) / groups
        move(part.at[j], gw.at[pl.ds(j * crows, crows)])
    for cp in moves:
        cp.wait()


def fused(n, groups, saved_input, queries, keys, value_weight, grad_attended):
    chips = groups // 2
    tokens, feat = saved_input.shape
    depth, width = value_weight.shape
    crows = feat // chips
    bf16 = jnp.bfloat16
    levels = n - 1
    vmem = pl.BlockSpec(memory_space=pltpu.VMEM)
    results = pl.pallas_call(
        functools.partial(fused_kernel, n, chips),
        out_shape=(
            pltpu.VMEM((tokens, feat), bf16),
            pltpu.VMEM((chips // 2, crows, width), bf16),
            pltpu.VMEM(queries.shape, bf16),
            pltpu.VMEM(keys.shape, bf16),
        ),
        in_specs=[pl.BlockSpec(memory_space=pl.ANY)] * 5,
        out_specs=(vmem,) * 4,
        scratch_shapes=[
            pltpu.VMEM((2 * tokens, feat), bf16),
            pltpu.VMEM(queries.shape, bf16),
            pltpu.VMEM(keys.shape, bf16),
            pltpu.VMEM(grad_attended.shape, bf16),
            pltpu.VMEM((n, feat, width), bf16),
            pltpu.VMEM((n, 2 * tokens, width), bf16),
            pltpu.VMEM((feat, 2 * tokens), bf16),
            pltpu.VMEM((n, 2, chips // 2, crows, width), bf16),
            pltpu.VMEM((n, 2, crows // 2, width), bf16),
            pltpu.VMEM((n, 2, crows // 2, width), bf16),
            pltpu.VMEM((n, 2, crows // 2, width), bf16),
            pltpu.VMEM((n, crows // 2, width), bf16),
            pltpu.VMEM((n, crows // 2, width), bf16),
            pltpu.VMEM((n, crows, width), bf16),
            pltpu.VMEM((2, tokens, width), jnp.float32),
            pltpu.VMEM((levels, 2 * tokens, width), bf16),
            pltpu.VMEM((levels, tokens, width), bf16),
            pltpu.VMEM((2, 2 * tokens, width), bf16),
            pltpu.VMEM((width // HD, tokens, tokens), jnp.float32),
            pltpu.VMEM((levels, crows, width), bf16),
            pltpu.SemaphoreType.DMA((160,)),
            pltpu.SemaphoreType.DMA((96,)),
            pltpu.SemaphoreType.DMA((8,)),
        ],
        compiler_params=pltpu.CompilerParams(
            collective_id=0, has_side_effects=True, vmem_limit_bytes=58 * 2**20
        ),
    )(saved_input, queries, keys, value_weight, grad_attended)
    outs = (
        (saved_input.shape, bf16), ((depth // groups, width), jnp.float32),
        (queries.shape, bf16), (keys.shape, bf16),
    )
    return pl.pallas_call(
        functools.partial(write_out, float(groups)),
        out_shape=tuple(jax.ShapeDtypeStruct(*out) for out in outs),
        in_specs=[vmem] * 4,
        out_specs=(pl.BlockSpec(memory_space=pl.ANY),) * 4,
        scratch_shapes=[
            pltpu.VMEM((chips // 2, crows, width), jnp.float32),
            pltpu.SemaphoreType.DMA((3 + chips // 2,)),
        ],
        compiler_params=pltpu.CompilerParams(vmem_limit_bytes=8 * 2**20),
    )(*results)


def on_device(saved_input, queries, keys, value_weight, grad_attended):
    token_count = queries.shape[0]
    local_width = value_weight.shape[1]
    local_heads = local_width // HD
    score_scale = 1.0 / jnp.sqrt(jnp.float32(HD))
    full_input = lax.all_gather(saved_input, "tensor", axis=1, tiled=True)
    values = jnp.dot(full_input, value_weight, preferred_element_type=jnp.float32).astype(
        jnp.bfloat16
    )
    query_heads = queries.reshape(token_count, local_heads, HD)
    key_heads = keys.reshape(token_count, local_heads, HD)
    value_heads = values.reshape(token_count, local_heads, HD)
    grad_heads = grad_attended.reshape(token_count, local_heads, HD)
    scores = (
        jnp.einsum("qhd,khd->hqk", query_heads, key_heads, preferred_element_type=jnp.float32)
        * score_scale
    )
    positions = lax.iota(jnp.int32, token_count)
    causal = positions[:, None] >= positions[None, :]
    scores = jnp.where(causal[None], scores, -jnp.inf)
    row_max = jnp.max(scores, axis=-1, keepdims=True)
    weights_exp = jnp.exp(scores - row_max)
    attention = weights_exp / jnp.sum(weights_exp, axis=-1, keepdims=True)
    probs_half = attention.astype(jnp.bfloat16)
    grad_values = jnp.einsum(
        "hqk,qhd->khd", probs_half, grad_heads, preferred_element_type=jnp.float32
    ).astype(jnp.bfloat16)
    grad_probs = jnp.einsum(
        "qhd,khd->hqk", grad_heads, value_heads, preferred_element_type=jnp.float32
    )
    row_dot = jnp.sum(attention * grad_probs, axis=-1, keepdims=True)
    grad_scores = (attention * (grad_probs - row_dot) * score_scale).astype(jnp.bfloat16)
    grad_queries = jnp.einsum(
        "hqk,khd->qhd", grad_scores, key_heads, preferred_element_type=jnp.float32
    ).astype(jnp.bfloat16)
    grad_keys = jnp.einsum(
        "hqk,qhd->khd", grad_scores, query_heads, preferred_element_type=jnp.float32
    ).astype(jnp.bfloat16)
    value_flat = grad_values.reshape(token_count, local_width)
    data_groups = lax.axis_size("dp")
    partial_value = lax.dot_general(
        value_flat, value_weight, (((1,), (1,)), ((), ())), preferred_element_type=jnp.float32
    )
    grad_input = lax.psum_scatter(
        partial_value.astype(jnp.bfloat16), "tensor", scatter_dimension=1, tiled=True
    )
    partial_value = lax.dot_general(
        full_input, value_flat, (((0,), (0,)), ((), ())), preferred_element_type=jnp.float32
    )
    summed = lax.psum_scatter(
        partial_value.astype(jnp.bfloat16), "dp", scatter_dimension=0, tiled=True
    ).astype(jnp.float32)
    grad_value_weight = summed / jnp.float32(data_groups)
    return (
        grad_input,
        grad_value_weight,
        grad_queries.reshape(token_count, local_width),
        grad_keys.reshape(token_count, local_width),
    )


def solution(mesh):
    placed = (
        P("dp", "tensor"),
        P("dp", "tensor"),
        P("dp", "tensor"),
        P(None, "tensor"),
        P("dp", "tensor"),
    )
    levels, groups = mesh.shape["tensor"], mesh.shape["dp"]
    run = on_device
    if groups == 2 * levels and levels == 4:
        run = functools.partial(fused, levels, groups)
    return jax.shard_map(
        run,
        mesh=mesh,
        in_specs=placed,
        out_specs=(P("dp", "tensor"), P("dp", "tensor"), P("dp", "tensor"), P("dp", "tensor")),
        check_vma=False,
    )
```

```python
import functools
import math

import jax
import jax.numpy as jnp
from jax import lax
from jax.experimental import pallas as pl
from jax.experimental.pallas import tpu as pltpu
from jax.sharding import PartitionSpec as P

HD = 128
END_WEIGHT = (
    ("W", 2), ("W", 3), ("W", 1), ("start", 0), ("sp", 2), ("sp", 1), ("on", 2), ("x", 0),
    ("sp", 3), ("end", 2), ("on", 3), ("vp", 2), ("end", 3), ("vp", 3), ("on", 1),
    ("end", 1), ("vp", 1), ("fin", 0),
)
MIDDLE_WEIGHT = (
    ("W", 1), ("W", 3), ("start", 0), ("W", 2), ("sp", 2), ("sp", 3), ("on", 2), ("sp", 1),
    ("on", 3), ("end", 2), ("on", 1), ("x", 0), ("end", 1), ("vp", 2), ("end", 3),
    ("vp", 1), ("vp", 3), ("cs", 3), ("fin", 0),
)
END_GRAD = (
    ("tk", 1), ("start", 0), ("twin", 0), ("x", 0), ("wt", 0), ("gvm", 0), ("gvt", 0),
    ("tk", 2), ("s2", 0), ("wt", 2), ("wt", 1), ("s2", 2), ("tk", 3), ("wt", 3), ("f", 2),
    ("s2", 3), ("s2", 1), ("f", 0), ("f", 3), ("f", 1), ("fin", 0),
)
MIDDLE_GRAD = (
    ("gvm", 0), ("start", 0), ("twin", 0), ("gvt", 0), ("x", 0), ("wt", 0), ("tk", 1),
    ("tk", 3), ("wt", 3), ("wt", 1), ("tk", 2), ("s2", 3), ("wt", 2), ("s2", 1), ("f", 3),
    ("s2", 0), ("s2", 2), ("f", 0), ("f", 1), ("f", 2), ("fin", 0),
)
JOINED = (3,)


def fused_kernel(
    n, chips,
    x_hbm, q_hbm, k_hbm, w, ga_hbm,
    gi, fin, gq, gk,
    x, queries, keys, ga,
    wfull, gvall, xt, qs, r1x, r1y, t2, r2x, r2y, zs,
    part, vsend, vrecv, vsum, probs, wsend,
    send_sem, recv_sem, load_sem,
):
    f32, bf16 = jnp.float32, jnp.bfloat16
    tokens, width = queries.shape
    feat = x.shape[1]
    crows = feat // chips
    hr = crows // 2
    heads = width // HD
    t = lax.axis_index("tensor")
    d = lax.axis_index("dp")
    c, k = d // 2, d % 2
    cx, cy = c % 2, c // 2
    scale = 1.0 / (HD ** 0.5)
    last = n - 1
    upper = t // (n // 2)
    edge = (t % last) == 0
    mid = (t % last) != 0
    level = [t, t + 1 - 2 * (t % 2), last - last * upper, n // 2 - upper]

    def at(s):
        return (d, s)

    partner = (d + 1 - 2 * k, t)
    xn = (d + 2 - 4 * cx, t)
    yn = (d + 4 - 8 * cy, t)
    diagonal = (d + 2 - 4 * cx + 4 - 8 * cy, t)
    chip_x, chip_y, chip_d = c + 1 - 2 * cx, c + 2 - 4 * cy, last - c

    counts = [0, 0]
    sent = {}
    now = [None]

    def slot():
        counts[1] += 1
        return counts[1] - 1

    def slots():
        return [slot() for _ in range(n)]

    def copy(src, dst, device, recv):
        i = counts[0]
        counts[0] += 1
        cp = pltpu.make_async_remote_copy(
            src_ref=src, dst_ref=dst, send_sem=send_sem.at[i], recv_sem=recv_sem.at[recv],
            device_id=device, device_id_type=pl.DeviceIdType.MESH,
        )
        cp.start()
        sent.setdefault(now[0], []).append((i, math.prod(src.shape) * src.dtype.itemsize // (2 * width)))

    def drain(name):
        for i, size in sent[name]:
            ref = wfull.at[0, 0:size]
            pltpu.make_async_remote_copy(
                src_ref=ref, dst_ref=ref, send_sem=send_sem.at[i], recv_sem=recv_sem.at[0],
                device_id=partner, device_id_type=pl.DeviceIdType.MESH,
            ).wait_send()

    def arrive(recv, ref):
        pltpu.make_async_remote_copy(
            src_ref=ref, dst_ref=ref, send_sem=send_sem.at[0], recv_sem=recv_sem.at[recv],
            device_id=partner, device_id_type=pl.DeviceIdType.MESH,
        ).wait_recv()

    def rows(i, size):
        return pl.ds(pl.multiple_of(i * size, size), size)

    mine, theirs = rows(k, tokens), rows(1 - k, tokens)

    barrier = pltpu.get_barrier_semaphore()
    peers = [at((t + o) % n) for o in range(1, n)] + [xn, yn, diagonal, partner]
    for peer in peers:
        pl.semaphore_signal(
            barrier, inc=1, device_id=peer, device_id_type=pl.DeviceIdType.MESH
        )
    ahead = [
        pltpu.make_async_copy(
            w.at[pl.ds(pl.multiple_of(level[i] * feat + c * crows, crows), crows)],
            wsend.at[i - 1], load_sem.at[4 + i],
        )
        for i in range(1, n)
    ]
    loads = [
        pltpu.make_async_copy(src, dst, load_sem.at[i])
        for i, (src, dst) in enumerate([
            (q_hbm, queries), (k_hbm, keys), (ga_hbm, ga), (x_hbm, x.at[mine]),
            (w.at[rows(t, feat)], wfull.at[t]),
        ])
    ]

    @pl.when(k == 0)
    def _():
        for load in ahead:
            load.start()
    for load in loads[:4]:
        load.start()

    def attend():
        for load in loads[:3]:
            load.wait()
        row = lax.broadcasted_iota(jnp.int32, (tokens, tokens), 0)
        col = lax.broadcasted_iota(jnp.int32, (tokens, tokens), 1)
        causal = row >= col
        for h in range(heads):
            cols = slice(h * HD, (h + 1) * HD)
            scores = lax.dot_general(
                queries[:, cols], keys[:, cols], (((1,), (1,)), ((), ())),
                preferred_element_type=f32,
            ) * scale
            scores = jnp.where(causal, scores, -jnp.inf)
            e = jnp.exp(scores - jnp.max(scores, axis=-1, keepdims=True))
            p = e / jnp.sum(e, axis=-1, keepdims=True)
            probs[h] = p
            gvall[t, mine, cols] = lax.dot_general(
                p.astype(bf16), ga[:, cols], (((0,), (0,)), ((), ())),
                preferred_element_type=f32,
            ).astype(bf16)
        loads[3].wait()
        loads[4].start()

    def everyone():
        pl.semaphore_wait(barrier, len(peers))

    xs, gvs, ws, vs = slot(), slots(), slots(), slot()
    gza, gzb = slots(), slots()
    wz, wpx, wpy, wqx, wqy, wrx, wry = (slots() for _ in range(7))
    p1x, p1y, p2x, p2y = slots(), slots(), slots(), slots()
    vz, pc = slots(), slots()
    fs = [[slot() for _ in range(chips // 2)] for _ in range(2)]
    home = c == t
    here = jnp.logical_and(home, cy == 1)
    away = jnp.logical_not(here)
    contract = (((1,), (1,)), ((), ()))

    def grad_in():
        acc = lax.dot_general(
            gvall[t, mine, :], wfull[t], contract, preferred_element_type=f32
        )
        for i in range(1, n):
            acc = acc + lax.dot_general(
                gvall[level[i], mine, :], wfull[level[i]], contract,
                preferred_element_type=f32,
            )
        gi[...] = acc.astype(bf16)

    def chunk(i, who, first=0, size=crows):
        start = pl.multiple_of(who * crows, crows) + first
        return wfull.at[level[i], pl.ds(pl.multiple_of(start, hr), size)]

    def weight_chain(end):
        for load in ahead:
            load.wait()
        everyone()

        def send_weight(i):
            copy(
                wsend.at[i - 1],
                wfull.at[t, rows(c, crows)],
                at(level[i]),
                wz[1] if i == 1 else wz[2] if end else wz[3],
            )

        def start(_):
            attend()
            copy(gvall.at[t, mine], gvall.at[t, mine], partner, gvs[0])
            copy(x.at[mine], x.at[mine], partner, xs)

        def spread(i):
            arrive(wz[i], chunk(i, c))
            low, high = chunk(i, c, 0, hr), chunk(i, c, hr, hr)
            copy(high, high, xn, wpx[i])
            copy(low, low, yn, wpy[i])
            copy(low, low, xn, wqx[i])
            copy(high, high, yn, wqy[i])

        def spread_on(i):
            piece = chunk(i, chip_x, hr, hr)
            arrive(wpx[i], piece)
            copy(piece, piece, yn, wry[i])
            piece = chunk(i, chip_y, 0, hr)
            arrive(wpy[i], piece)
            copy(piece, piece, xn, wrx[i])

        def spread_end(i):
            arrive(wqx[i], chunk(i, chip_x, 0, hr))
            arrive(wqy[i], chunk(i, chip_y, hr, hr))
            arrive(wrx[i], chunk(i, chip_d, 0, hr))
            arrive(wry[i], chunk(i, chip_d, hr, hr))
            copy(wfull.at[level[i]], wfull.at[level[i]], partner, ws[i])

        def value_send(i, seen):
            for j in range(2):
                copy(
                    vsend.at[i - 1, rows(j, tokens)], vrecv.at[seen - 1],
                    (2 * c + j, level[i]), vz[seen],
                )

        def value_part(i):
            vsend[i - 1] = jnp.dot(
                x[...], wfull[level[i]], preferred_element_type=f32
            ).astype(bf16)
            if i not in JOINED:
                value_send(i, 1 if i == 1 else 2 if end else 3)
            elif end:
                copy(vsend.at[i - 1], vsum.at[i - 2], at(level[1]), pc[i])

        def value_join(i):
            arrive(pc[i], vsum.at[i - 2])
            vsend[i - 1] = (vsend[i - 1].astype(f32) + vsum[i - 2].astype(f32)).astype(bf16)
            value_send(i, 3)

        def close(_):
            loads[4].wait()
            own = jnp.dot(x[...], wfull[t], preferred_element_type=f32)
            part[0] = own[0:tokens]
            part[1] = own[tokens:2 * tokens]
            copy(part.at[1], part.at[0], partner, vs)
            for i in range(1, n):
                arrive(gvs[i], gvall.at[glevel(end, i), mine])
            grad_in()
            gather(end)

        steps = {
            "W": send_weight, "start": start, "sp": spread, "on": spread_on,
            "end": spread_end, "vp": value_part, "cs": value_join, "fin": close,
            "x": lambda _: arrive(xs, x.at[theirs]),
        }
        for op, i in END_WEIGHT if end else MIDDLE_WEIGHT:
            steps[op](i)

    def gather(end):
        total = part[0]
        for i in range(1, n):
            if i != 2 or (2 if end else 3) not in JOINED:
                arrive(vz[i], vrecv.at[i - 1])
                total = total + vrecv[i - 1].astype(f32)
        part[0] = total

    def glevel(end, i):
        return level[(0, 1, 3, 2)[i] if end else (0, 3, 1, 2)[i]]

    def grad_chain(end):
        def gv(i, which):
            return gvall.at[glevel(end, i), which]

        def send_gv(which, sem):
            for to, got in ((1, 2), (3, 3)) if end else ((3, 1), (1, 1)):
                copy(gv(0, which), gv(0, which), at(level[to]), sem[got])

        attend()
        everyone()
        def start(_):
            copy(x.at[mine], x.at[mine], partner, xs)

        def turn(_):
            xt[:, mine] = x[mine, :].T
            arrive(xs, x.at[theirs])
            xt[:, theirs] = x[theirs, :].T

        def take(i):
            for which, sem in ((mine, gza), (theirs, gzb)):
                arrive(sem[i], gv(i, which))
                if not end and i != 2:
                    copy(gv(i, which), gv(i, which), at(level[1]), sem[(2, 2, 2, 3)[i]])
            copy(gv(i, theirs), gv(i, theirs), partner, gvs[i])

        def weight_term(i):
            term = jnp.dot(
                xt[...], gvall[glevel(end, i)], preferred_element_type=f32
            ).astype(bf16)
            for j in range(chips):
                qs[i, j // 2, j % 2] = term[j * crows:(j + 1) * crows]
            copy(qs.at[i, :, 1 - cx, 0:hr, :], r1x.at[i], xn, p1x[i])
            copy(qs.at[i, 1 - cy, :, hr:crows, :], r1y.at[i], yn, p1y[i])

        def second_phase(i):
            arrive(p1x[i], r1x.at[i])
            t2[i, 0] = (
                qs[i, 1 - cy, cx, 0:hr, :].astype(f32) + r1x[i, 1 - cy].astype(f32)
            ).astype(bf16)
            copy(t2.at[i, 0], r2y.at[i], yn, p2y[i])
            arrive(p1y[i], r1y.at[i])
            t2[i, 1] = (
                qs[i, cy, 1 - cx, hr:crows, :].astype(f32) + r1y[i, 1 - cx].astype(f32)
            ).astype(bf16)
            copy(t2.at[i, 1], r2x.at[i], xn, p2x[i])

        def finish(i):
            for j, (mine_in, first, second) in enumerate((
                (p2y[i], r1x[i, cy], r2y), (p2x[i], r1y[i, cx], r2x),
            )):
                part_rows = slice(j * hr, (j + 1) * hr)
                arrive(mine_in, second.at[i])
                zs[i, part_rows, :] = (
                    qs[i, cy, cx, part_rows, :].astype(f32) + first.astype(f32)
                    + second[i].astype(f32)
                ).astype(bf16)
                if i > 0:
                    copy(
                        zs.at[i, part_rows], fin.at[cx, part_rows],
                        (2 * t + cy, glevel(end, i)), fs[j][0] + cx,
                    )
                else:
                    @pl.when(here)
                    def _():
                        fin[cx, part_rows] = zs[0, part_rows]

                    @pl.when(away)
                    def _():
                        own_final(j).start()

        def close(_):
            loads[4].wait()
            for i in range(1, n):
                arrive(ws[i], wfull.at[level[i]])
            grad_in()
            arrive(vs, part.at[0])
            gather(end)

        steps = {
            "start": start, "x": turn, "tk": take, "wt": weight_term, "s2": second_phase,
            "f": finish, "fin": close,
            "twin": lambda _: arrive(gvs[0], gv(0, theirs)),
            "gvm": lambda _: send_gv(mine, gza),
            "gvt": lambda _: send_gv(theirs, gzb),
        }
        for op, i in END_GRAD if end else MIDDLE_GRAD:
            steps[op](i)

    def own_final(j):
        part_rows = slice(j * hr, (j + 1) * hr)
        return pltpu.make_async_remote_copy(
            src_ref=zs.at[0, part_rows], dst_ref=fin.at[cx, part_rows],
            send_sem=send_sem.at[send_sem.shape[0] - 1 - j],
            recv_sem=recv_sem.at[fs[j][0] + cx],
            device_id=(2 * t + cy, t), device_id_type=pl.DeviceIdType.MESH,
        )

    for role, chain in enumerate((weight_chain, grad_chain)):
        for end in (True, False):
            now[0] = (role, end)

            @pl.when(jnp.logical_and(k == role, edge if end else mid))
            def _():
                chain(end)

    values = part[0].astype(bf16)
    for h in range(heads):
        cols = slice(h * HD, (h + 1) * HD)
        grad_probs = lax.dot_general(
            ga[:, cols], values[:, cols], contract, preferred_element_type=f32
        )
        p = probs[h]
        row_dot = jnp.sum(p * grad_probs, axis=-1, keepdims=True)
        gs = (p * (grad_probs - row_dot) * scale).astype(bf16)
        gq[:, cols] = jnp.dot(gs, keys[:, cols], preferred_element_type=f32).astype(bf16)
        gk[:, cols] = lax.dot_general(
            gs, queries[:, cols], (((0,), (0,)), ((), ())), preferred_element_type=f32
        ).astype(bf16)

    for j in range(chips // 2):
        local = jnp.logical_and(here, jnp.logical_and(k == 1, cx == j))

        @pl.when(jnp.logical_not(local))
        def _():
            for h in range(2):
                arrive(fs[h][j], fin.at[j, h * hr:(h + 1) * hr])

    @pl.when(jnp.logical_and(k == 1, away))
    def _():
        for j in range(2):
            own_final(j).wait_send()

    for role in range(2):
        for end in (True, False):
            @pl.when(jnp.logical_and(k == role, edge if end else mid))
            def _():
                drain((role, end))
    assert counts[0] < send_sem.shape[0] - 1 and counts[1] <= recv_sem.shape[0], counts


def write_out(groups, gi_in, fin, gq_in, gk_in, gi, gw, gq, gk, part, sem):
    crows = fin.shape[1]
    moves = []

    def move(src, dst):
        cp = pltpu.make_async_copy(src, dst, sem.at[len(moves)])
        cp.start()
        moves.append(cp)

    move(gi_in, gi)
    move(gq_in, gq)
    move(gk_in, gk)
    for j in range(fin.shape[0]):
        part[j] = fin[j].astype(jnp.float32) / groups
        move(part.at[j], gw.at[pl.ds(j * crows, crows)])
    for cp in moves:
        cp.wait()


def fused(n, groups, saved_input, queries, keys, value_weight, grad_attended):
    chips = groups // 2
    tokens, feat = saved_input.shape
    depth, width = value_weight.shape
    crows = feat // chips
    bf16 = jnp.bfloat16
    levels = n - 1
    vmem = pl.BlockSpec(memory_space=pltpu.VMEM)
    results = pl.pallas_call(
        functools.partial(fused_kernel, n, chips),
        out_shape=(
            pltpu.VMEM((tokens, feat), bf16),
            pltpu.VMEM((chips // 2, crows, width), bf16),
            pltpu.VMEM(queries.shape, bf16),
            pltpu.VMEM(keys.shape, bf16),
        ),
        in_specs=[pl.BlockSpec(memory_space=pl.ANY)] * 5,
        out_specs=(vmem,) * 4,
        scratch_shapes=[
            pltpu.VMEM((2 * tokens, feat), bf16),
            pltpu.VMEM(queries.shape, bf16),
            pltpu.VMEM(keys.shape, bf16),
            pltpu.VMEM(grad_attended.shape, bf16),
            pltpu.VMEM((n, feat, width), bf16),
            pltpu.VMEM((n, 2 * tokens, width), bf16),
            pltpu.VMEM((feat, 2 * tokens), bf16),
            pltpu.VMEM((n, 2, chips // 2, crows, width), bf16),
            pltpu.VMEM((n, 2, crows // 2, width), bf16),
            pltpu.VMEM((n, 2, crows // 2, width), bf16),
            pltpu.VMEM((n, 2, crows // 2, width), bf16),
            pltpu.VMEM((n, crows // 2, width), bf16),
            pltpu.VMEM((n, crows // 2, width), bf16),
            pltpu.VMEM((n, crows, width), bf16),
            pltpu.VMEM((2, tokens, width), jnp.float32),
            pltpu.VMEM((levels, 2 * tokens, width), bf16),
            pltpu.VMEM((levels, tokens, width), bf16),
            pltpu.VMEM((2, 2 * tokens, width), bf16),
            pltpu.VMEM((width // HD, tokens, tokens), jnp.float32),
            pltpu.VMEM((levels, crows, width), bf16),
            pltpu.SemaphoreType.DMA((192,)),
            pltpu.SemaphoreType.DMA((96,)),
            pltpu.SemaphoreType.DMA((8,)),
        ],
        compiler_params=pltpu.CompilerParams(
            collective_id=0, has_side_effects=True, vmem_limit_bytes=58 * 2**20
        ),
    )(saved_input, queries, keys, value_weight, grad_attended)
    outs = (
        (saved_input.shape, bf16), ((depth // groups, width), jnp.float32),
        (queries.shape, bf16), (keys.shape, bf16),
    )
    return pl.pallas_call(
        functools.partial(write_out, float(groups)),
        out_shape=tuple(jax.ShapeDtypeStruct(*out) for out in outs),
        in_specs=[vmem] * 4,
        out_specs=(pl.BlockSpec(memory_space=pl.ANY),) * 4,
        scratch_shapes=[
            pltpu.VMEM((chips // 2, crows, width), jnp.float32),
            pltpu.SemaphoreType.DMA((3 + chips // 2,)),
        ],
        compiler_params=pltpu.CompilerParams(vmem_limit_bytes=8 * 2**20),
    )(*results)


def on_device(saved_input, queries, keys, value_weight, grad_attended):
    token_count = queries.shape[0]
    local_width = value_weight.shape[1]
    local_heads = local_width // HD
    score_scale = 1.0 / jnp.sqrt(jnp.float32(HD))
    full_input = lax.all_gather(saved_input, "tensor", axis=1, tiled=True)
    values = jnp.dot(full_input, value_weight, preferred_element_type=jnp.float32).astype(
        jnp.bfloat16
    )
    query_heads = queries.reshape(token_count, local_heads, HD)
    key_heads = keys.reshape(token_count, local_heads, HD)
    value_heads = values.reshape(token_count, local_heads, HD)
    grad_heads = grad_attended.reshape(token_count, local_heads, HD)
    scores = (
        jnp.einsum("qhd,khd->hqk", query_heads, key_heads, preferred_element_type=jnp.float32)
        * score_scale
    )
    positions = lax.iota(jnp.int32, token_count)
    causal = positions[:, None] >= positions[None, :]
    scores = jnp.where(causal[None], scores, -jnp.inf)
    row_max = jnp.max(scores, axis=-1, keepdims=True)
    weights_exp = jnp.exp(scores - row_max)
    attention = weights_exp / jnp.sum(weights_exp, axis=-1, keepdims=True)
    probs_half = attention.astype(jnp.bfloat16)
    grad_values = jnp.einsum(
        "hqk,qhd->khd", probs_half, grad_heads, preferred_element_type=jnp.float32
    ).astype(jnp.bfloat16)
    grad_probs = jnp.einsum(
        "qhd,khd->hqk", grad_heads, value_heads, preferred_element_type=jnp.float32
    )
    row_dot = jnp.sum(attention * grad_probs, axis=-1, keepdims=True)
    grad_scores = (attention * (grad_probs - row_dot) * score_scale).astype(jnp.bfloat16)
    grad_queries = jnp.einsum(
        "hqk,khd->qhd", grad_scores, key_heads, preferred_element_type=jnp.float32
    ).astype(jnp.bfloat16)
    grad_keys = jnp.einsum(
        "hqk,qhd->khd", grad_scores, query_heads, preferred_element_type=jnp.float32
    ).astype(jnp.bfloat16)
    value_flat = grad_values.reshape(token_count, local_width)
    data_groups = lax.axis_size("dp")
    partial_value = lax.dot_general(
        value_flat, value_weight, (((1,), (1,)), ((), ())), preferred_element_type=jnp.float32
    )
    grad_input = lax.psum_scatter(
        partial_value.astype(jnp.bfloat16), "tensor", scatter_dimension=1, tiled=True
    )
    partial_value = lax.dot_general(
        full_input, value_flat, (((0,), (0,)), ((), ())), preferred_element_type=jnp.float32
    )
    summed = lax.psum_scatter(
        partial_value.astype(jnp.bfloat16), "dp", scatter_dimension=0, tiled=True
    ).astype(jnp.float32)
    grad_value_weight = summed / jnp.float32(data_groups)
    return (
        grad_input,
        grad_value_weight,
        grad_queries.reshape(token_count, local_width),
        grad_keys.reshape(token_count, local_width),
    )


def solution(mesh):
    placed = (
        P("dp", "tensor"),
        P("dp", "tensor"),
        P("dp", "tensor"),
        P(None, "tensor"),
        P("dp", "tensor"),
    )
    levels, groups = mesh.shape["tensor"], mesh.shape["dp"]
    run = on_device
    if groups == 2 * levels and levels == 4:
        run = functools.partial(fused, levels, groups)
    return jax.shard_map(
        run,
        mesh=mesh,
        in_specs=placed,
        out_specs=(P("dp", "tensor"), P("dp", "tensor"), P("dp", "tensor"), P("dp", "tensor")),
        check_vma=False,
    )
```

```python
import functools
import math

import jax
import jax.numpy as jnp
from jax import lax
from jax.experimental import pallas as pl
from jax.experimental.pallas import tpu as pltpu
from jax.sharding import PartitionSpec as P

HD = 128
END_WEIGHT = (
    ("W", 2), ("W", 3), ("W", 1), ("start", 0), ("sp", 2), ("sp", 1), ("on", 2), ("x", 0),
    ("sp", 3), ("end", 2), ("on", 3), ("vp", 2), ("end", 3), ("vp", 3), ("on", 1),
    ("end", 1), ("vp", 1), ("fin", 0),
)
MIDDLE_WEIGHT = (
    ("W", 1), ("W", 3), ("start", 0), ("W", 2), ("sp", 2), ("sp", 3), ("on", 2), ("sp", 1),
    ("on", 3), ("end", 2), ("on", 1), ("x", 0), ("end", 1), ("vp", 2), ("end", 3),
    ("vp", 1), ("vp", 3), ("cs", 3), ("fin", 0),
)
END_GRAD = (
    ("start", 0), ("twin", 0), ("tk", 1), ("x", 0), ("wt", 0), ("gvm", 0), ("gvt", 0),
    ("tk", 2), ("s2", 0), ("wt", 2), ("wt", 1), ("s2", 2), ("tk", 3), ("wt", 3), ("f", 2),
    ("s2", 3), ("s2", 1), ("f", 0), ("f", 3), ("f", 1), ("fin", 0),
)
MIDDLE_GRAD = (
    ("gvm", 0), ("start", 0), ("twin", 0), ("gvt", 0), ("x", 0), ("wt", 0), ("tk", 1),
    ("tk", 3), ("wt", 3), ("wt", 1), ("tk", 2), ("s2", 3), ("wt", 2), ("s2", 1), ("f", 3),
    ("s2", 0), ("s2", 2), ("f", 0), ("f", 1), ("f", 2), ("fin", 0),
)
JOINED = (3,)


def fused_kernel(
    n, chips,
    x_hbm, q_hbm, k_hbm, w, ga_hbm,
    gi, fin, gq, gk,
    x, queries, keys, ga,
    wfull, gvall, xt, qs, r1x, r1y, t2, r2x, r2y, zs,
    part, vsend, vrecv, vsum, probs, wsend,
    send_sem, recv_sem, load_sem,
):
    f32, bf16 = jnp.float32, jnp.bfloat16
    tokens, width = queries.shape
    feat = x.shape[1]
    crows = feat // chips
    hr = crows // 2
    heads = width // HD
    t = lax.axis_index("tensor")
    d = lax.axis_index("dp")
    c, k = d // 2, d % 2
    cx, cy = c % 2, c // 2
    scale = 1.0 / (HD ** 0.5)
    last = n - 1
    upper = t // (n // 2)
    edge = (t % last) == 0
    mid = (t % last) != 0
    level = [t, t + 1 - 2 * (t % 2), last - last * upper, n // 2 - upper]

    def at(s):
        return (d, s)

    partner = (d + 1 - 2 * k, t)
    xn = (d + 2 - 4 * cx, t)
    yn = (d + 4 - 8 * cy, t)
    diagonal = (d + 2 - 4 * cx + 4 - 8 * cy, t)
    chip_x, chip_y, chip_d = c + 1 - 2 * cx, c + 2 - 4 * cy, last - c

    counts = [0, 0]
    sent = {}
    now = [None]

    def slot():
        counts[1] += 1
        return counts[1] - 1

    def slots():
        return [slot() for _ in range(n)]

    def copy(src, dst, device, recv):
        i = counts[0]
        counts[0] += 1
        cp = pltpu.make_async_remote_copy(
            src_ref=src, dst_ref=dst, send_sem=send_sem.at[i], recv_sem=recv_sem.at[recv],
            device_id=device, device_id_type=pl.DeviceIdType.MESH,
        )
        cp.start()
        sent.setdefault(now[0], []).append((i, math.prod(src.shape) * src.dtype.itemsize // (2 * width)))

    def drain(name):
        for i, size in sent[name]:
            ref = wfull.at[0, 0:size]
            pltpu.make_async_remote_copy(
                src_ref=ref, dst_ref=ref, send_sem=send_sem.at[i], recv_sem=recv_sem.at[0],
                device_id=partner, device_id_type=pl.DeviceIdType.MESH,
            ).wait_send()

    def arrive(recv, ref):
        pltpu.make_async_remote_copy(
            src_ref=ref, dst_ref=ref, send_sem=send_sem.at[0], recv_sem=recv_sem.at[recv],
            device_id=partner, device_id_type=pl.DeviceIdType.MESH,
        ).wait_recv()

    def rows(i, size):
        return pl.ds(pl.multiple_of(i * size, size), size)

    mine, theirs = rows(k, tokens), rows(1 - k, tokens)

    barrier = pltpu.get_barrier_semaphore()
    peers = [at((t + o) % n) for o in range(1, n)] + [xn, yn, diagonal, partner]
    for peer in peers:
        pl.semaphore_signal(
            barrier, inc=1, device_id=peer, device_id_type=pl.DeviceIdType.MESH
        )
    ahead = [
        pltpu.make_async_copy(
            w.at[pl.ds(pl.multiple_of(level[i] * feat + c * crows, crows), crows)],
            wsend.at[i - 1], load_sem.at[4 + i],
        )
        for i in range(1, n)
    ]
    loads = [
        pltpu.make_async_copy(src, dst, load_sem.at[i])
        for i, (src, dst) in enumerate([
            (q_hbm, queries), (k_hbm, keys), (ga_hbm, ga), (x_hbm, x.at[mine]),
            (w.at[rows(t, feat)], wfull.at[t]),
        ])
    ]

    @pl.when(k == 0)
    def _():
        for load in ahead:
            load.start()
    for load in loads[:4]:
        load.start()

    def attend():
        for load in loads[:3]:
            load.wait()
        row = lax.broadcasted_iota(jnp.int32, (tokens, tokens), 0)
        col = lax.broadcasted_iota(jnp.int32, (tokens, tokens), 1)
        causal = row >= col
        for h in range(heads):
            cols = slice(h * HD, (h + 1) * HD)
            scores = lax.dot_general(
                queries[:, cols], keys[:, cols], (((1,), (1,)), ((), ())),
                preferred_element_type=f32,
            ) * scale
            scores = jnp.where(causal, scores, -jnp.inf)
            e = jnp.exp(scores - jnp.max(scores, axis=-1, keepdims=True))
            p = e / jnp.sum(e, axis=-1, keepdims=True)
            probs[h] = p
            gvall[t, mine, cols] = lax.dot_general(
                p.astype(bf16), ga[:, cols], (((0,), (0,)), ((), ())),
                preferred_element_type=f32,
            ).astype(bf16)
        loads[3].wait()
        loads[4].start()

    def everyone():
        pl.semaphore_wait(barrier, len(peers))

    xs, gvs, ws, vs = slot(), slots(), slots(), slot()
    gza, gzb = slots(), slots()
    wz, wpx, wpy, wqx, wqy, wrx, wry = (slots() for _ in range(7))
    p1x, p1y, p2x, p2y = slots(), slots(), slots(), slots()
    vz, pc = slots(), slots()
    fs = [[slot() for _ in range(chips // 2)] for _ in range(2)]
    home = c == t
    here = jnp.logical_and(home, cy == 1)
    away = jnp.logical_not(here)
    contract = (((1,), (1,)), ((), ()))

    def grad_in():
        acc = lax.dot_general(
            gvall[t, mine, :], wfull[t], contract, preferred_element_type=f32
        )
        for i in range(1, n):
            acc = acc + lax.dot_general(
                gvall[level[i], mine, :], wfull[level[i]], contract,
                preferred_element_type=f32,
            )
        gi[...] = acc.astype(bf16)

    def chunk(i, who, first=0, size=crows):
        start = pl.multiple_of(who * crows, crows) + first
        return wfull.at[level[i], pl.ds(pl.multiple_of(start, hr), size)]

    def weight_chain(end):
        for load in ahead:
            load.wait()
        everyone()

        def send_weight(i):
            copy(
                wsend.at[i - 1],
                wfull.at[t, rows(c, crows)],
                at(level[i]),
                wz[1] if i == 1 else wz[2] if end else wz[3],
            )

        def start(_):
            attend()
            copy(gvall.at[t, mine], gvall.at[t, mine], partner, gvs[0])
            copy(x.at[mine], x.at[mine], partner, xs)

        def spread(i):
            arrive(wz[i], chunk(i, c))
            low, high = chunk(i, c, 0, hr), chunk(i, c, hr, hr)
            copy(high, high, xn, wpx[i])
            copy(low, low, yn, wpy[i])
            copy(low, low, xn, wqx[i])
            copy(high, high, yn, wqy[i])

        def spread_on(i):
            piece = chunk(i, chip_x, hr, hr)
            arrive(wpx[i], piece)
            copy(piece, piece, yn, wry[i])
            piece = chunk(i, chip_y, 0, hr)
            arrive(wpy[i], piece)
            copy(piece, piece, xn, wrx[i])

        def spread_end(i):
            arrive(wqx[i], chunk(i, chip_x, 0, hr))
            arrive(wqy[i], chunk(i, chip_y, hr, hr))
            arrive(wrx[i], chunk(i, chip_d, 0, hr))
            arrive(wry[i], chunk(i, chip_d, hr, hr))
            copy(wfull.at[level[i]], wfull.at[level[i]], partner, ws[i])

        def value_send(i, seen):
            for j in range(2):
                copy(
                    vsend.at[i - 1, rows(j, tokens)], vrecv.at[seen - 1],
                    (2 * c + j, level[i]), vz[seen],
                )

        def value_part(i):
            vsend[i - 1] = jnp.dot(
                x[...], wfull[level[i]], preferred_element_type=f32
            ).astype(bf16)
            if i not in JOINED:
                value_send(i, 1 if i == 1 else 2 if end else 3)
            elif end:
                copy(vsend.at[i - 1], vsum.at[i - 2], at(level[1]), pc[i])

        def value_join(i):
            arrive(pc[i], vsum.at[i - 2])
            vsend[i - 1] = (vsend[i - 1].astype(f32) + vsum[i - 2].astype(f32)).astype(bf16)
            value_send(i, 3)

        def close(_):
            loads[4].wait()
            own = jnp.dot(x[...], wfull[t], preferred_element_type=f32)
            part[0] = own[0:tokens]
            part[1] = own[tokens:2 * tokens]
            copy(part.at[1], part.at[0], partner, vs)
            for i in range(1, n):
                arrive(gvs[i], gvall.at[glevel(end, i), mine])
            grad_in()
            gather(end)

        steps = {
            "W": send_weight, "start": start, "sp": spread, "on": spread_on,
            "end": spread_end, "vp": value_part, "cs": value_join, "fin": close,
            "x": lambda _: arrive(xs, x.at[theirs]),
        }
        for op, i in END_WEIGHT if end else MIDDLE_WEIGHT:
            steps[op](i)

    def gather(end):
        total = part[0]
        for i in range(1, n):
            if i != 2 or (2 if end else 3) not in JOINED:
                arrive(vz[i], vrecv.at[i - 1])
                total = total + vrecv[i - 1].astype(f32)
        part[0] = total

    def glevel(end, i):
        return level[(0, 1, 3, 2)[i] if end else (0, 3, 1, 2)[i]]

    def grad_chain(end):
        def gv(i, which):
            return gvall.at[glevel(end, i), which]

        def send_gv(which, sem):
            for to, got in ((1, 2), (3, 3)) if end else ((3, 1), (1, 1)):
                copy(gv(0, which), gv(0, which), at(level[to]), sem[got])

        attend()
        everyone()
        def start(_):
            copy(x.at[mine], x.at[mine], partner, xs)

        def turn(_):
            xt[:, mine] = x[mine, :].T
            arrive(xs, x.at[theirs])
            xt[:, theirs] = x[theirs, :].T

        def take(i):
            for which, sem in ((mine, gza), (theirs, gzb)):
                arrive(sem[i], gv(i, which))
                if not end and i != 2:
                    copy(gv(i, which), gv(i, which), at(level[1]), sem[(2, 2, 2, 3)[i]])
            copy(gv(i, theirs), gv(i, theirs), partner, gvs[i])

        def weight_term(i):
            term = jnp.dot(
                xt[...], gvall[glevel(end, i)], preferred_element_type=f32
            ).astype(bf16)
            for j in range(chips):
                qs[i, j // 2, j % 2] = term[j * crows:(j + 1) * crows]
            copy(qs.at[i, :, 1 - cx, 0:hr, :], r1x.at[i], xn, p1x[i])
            copy(qs.at[i, 1 - cy, :, hr:crows, :], r1y.at[i], yn, p1y[i])

        def second_phase(i):
            arrive(p1x[i], r1x.at[i])
            t2[i, 0] = (
                qs[i, 1 - cy, cx, 0:hr, :].astype(f32) + r1x[i, 1 - cy].astype(f32)
            ).astype(bf16)
            copy(t2.at[i, 0], r2y.at[i], yn, p2y[i])
            arrive(p1y[i], r1y.at[i])
            t2[i, 1] = (
                qs[i, cy, 1 - cx, hr:crows, :].astype(f32) + r1y[i, 1 - cx].astype(f32)
            ).astype(bf16)
            copy(t2.at[i, 1], r2x.at[i], xn, p2x[i])

        def finish(i):
            for j, (mine_in, first, second) in enumerate((
                (p2y[i], r1x[i, cy], r2y), (p2x[i], r1y[i, cx], r2x),
            )):
                part_rows = slice(j * hr, (j + 1) * hr)
                arrive(mine_in, second.at[i])
                zs[i, part_rows, :] = (
                    qs[i, cy, cx, part_rows, :].astype(f32) + first.astype(f32)
                    + second[i].astype(f32)
                ).astype(bf16)
                if i > 0:
                    copy(
                        zs.at[i, part_rows], fin.at[cx, part_rows],
                        (2 * t + cy, glevel(end, i)), fs[j][0] + cx,
                    )
                else:
                    @pl.when(here)
                    def _():
                        fin[cx, part_rows] = zs[0, part_rows]

                    @pl.when(away)
                    def _():
                        own_final(j).start()

        def close(_):
            loads[4].wait()
            for i in range(1, n):
                arrive(ws[i], wfull.at[level[i]])
            grad_in()
            arrive(vs, part.at[0])
            gather(end)

        steps = {
            "start": start, "x": turn, "tk": take, "wt": weight_term, "s2": second_phase,
            "f": finish, "fin": close,
            "twin": lambda _: arrive(gvs[0], gv(0, theirs)),
            "gvm": lambda _: send_gv(mine, gza),
            "gvt": lambda _: send_gv(theirs, gzb),
        }
        for op, i in END_GRAD if end else MIDDLE_GRAD:
            steps[op](i)

    def own_final(j):
        part_rows = slice(j * hr, (j + 1) * hr)
        return pltpu.make_async_remote_copy(
            src_ref=zs.at[0, part_rows], dst_ref=fin.at[cx, part_rows],
            send_sem=send_sem.at[send_sem.shape[0] - 1 - j],
            recv_sem=recv_sem.at[fs[j][0] + cx],
            device_id=(2 * t + cy, t), device_id_type=pl.DeviceIdType.MESH,
        )

    for role, chain in enumerate((weight_chain, grad_chain)):
        for end in (True, False):
            now[0] = (role, end)

            @pl.when(jnp.logical_and(k == role, edge if end else mid))
            def _():
                chain(end)

    values = part[0].astype(bf16)
    for h in range(heads):
        cols = slice(h * HD, (h + 1) * HD)
        grad_probs = lax.dot_general(
            ga[:, cols], values[:, cols], contract, preferred_element_type=f32
        )
        p = probs[h]
        row_dot = jnp.sum(p * grad_probs, axis=-1, keepdims=True)
        gs = (p * (grad_probs - row_dot) * scale).astype(bf16)
        gq[:, cols] = jnp.dot(gs, keys[:, cols], preferred_element_type=f32).astype(bf16)
        gk[:, cols] = lax.dot_general(
            gs, queries[:, cols], (((0,), (0,)), ((), ())), preferred_element_type=f32
        ).astype(bf16)

    for j in range(chips // 2):
        local = jnp.logical_and(here, jnp.logical_and(k == 1, cx == j))

        @pl.when(jnp.logical_not(local))
        def _():
            for h in range(2):
                arrive(fs[h][j], fin.at[j, h * hr:(h + 1) * hr])

    @pl.when(jnp.logical_and(k == 1, away))
    def _():
        for j in range(2):
            own_final(j).wait_send()

    for role in range(2):
        for end in (True, False):
            @pl.when(jnp.logical_and(k == role, edge if end else mid))
            def _():
                drain((role, end))
    assert counts[0] < send_sem.shape[0] - 1 and counts[1] <= recv_sem.shape[0], counts


def write_out(groups, gi_in, fin, gq_in, gk_in, gi, gw, gq, gk, part, sem):
    crows = fin.shape[1]
    moves = []

    def move(src, dst):
        cp = pltpu.make_async_copy(src, dst, sem.at[len(moves)])
        cp.start()
        moves.append(cp)

    move(gi_in, gi)
    move(gq_in, gq)
    move(gk_in, gk)
    for j in range(fin.shape[0]):
        part[j] = fin[j].astype(jnp.float32) / groups
        move(part.at[j], gw.at[pl.ds(j * crows, crows)])
    for cp in moves:
        cp.wait()


def fused(n, groups, saved_input, queries, keys, value_weight, grad_attended):
    chips = groups // 2
    tokens, feat = saved_input.shape
    depth, width = value_weight.shape
    crows = feat // chips
    bf16 = jnp.bfloat16
    levels = n - 1
    vmem = pl.BlockSpec(memory_space=pltpu.VMEM)
    results = pl.pallas_call(
        functools.partial(fused_kernel, n, chips),
        out_shape=(
            pltpu.VMEM((tokens, feat), bf16),
            pltpu.VMEM((chips // 2, crows, width), bf16),
            pltpu.VMEM(queries.shape, bf16),
            pltpu.VMEM(keys.shape, bf16),
        ),
        in_specs=[pl.BlockSpec(memory_space=pl.ANY)] * 5,
        out_specs=(vmem,) * 4,
        scratch_shapes=[
            pltpu.VMEM((2 * tokens, feat), bf16),
            pltpu.VMEM(queries.shape, bf16),
            pltpu.VMEM(keys.shape, bf16),
            pltpu.VMEM(grad_attended.shape, bf16),
            pltpu.VMEM((n, feat, width), bf16),
            pltpu.VMEM((n, 2 * tokens, width), bf16),
            pltpu.VMEM((feat, 2 * tokens), bf16),
            pltpu.VMEM((n, 2, chips // 2, crows, width), bf16),
            pltpu.VMEM((n, 2, crows // 2, width), bf16),
            pltpu.VMEM((n, 2, crows // 2, width), bf16),
            pltpu.VMEM((n, 2, crows // 2, width), bf16),
            pltpu.VMEM((n, crows // 2, width), bf16),
            pltpu.VMEM((n, crows // 2, width), bf16),
            pltpu.VMEM((n, crows, width), bf16),
            pltpu.VMEM((2, tokens, width), jnp.float32),
            pltpu.VMEM((levels, 2 * tokens, width), bf16),
            pltpu.VMEM((levels, tokens, width), bf16),
            pltpu.VMEM((2, 2 * tokens, width), bf16),
            pltpu.VMEM((width // HD, tokens, tokens), jnp.float32),
            pltpu.VMEM((levels, crows, width), bf16),
            pltpu.SemaphoreType.DMA((192,)),
            pltpu.SemaphoreType.DMA((96,)),
            pltpu.SemaphoreType.DMA((8,)),
        ],
        compiler_params=pltpu.CompilerParams(
            collective_id=0, has_side_effects=True, vmem_limit_bytes=58 * 2**20
        ),
    )(saved_input, queries, keys, value_weight, grad_attended)
    outs = (
        (saved_input.shape, bf16), ((depth // groups, width), jnp.float32),
        (queries.shape, bf16), (keys.shape, bf16),
    )
    return pl.pallas_call(
        functools.partial(write_out, float(groups)),
        out_shape=tuple(jax.ShapeDtypeStruct(*out) for out in outs),
        in_specs=[vmem] * 4,
        out_specs=(pl.BlockSpec(memory_space=pl.ANY),) * 4,
        scratch_shapes=[
            pltpu.VMEM((chips // 2, crows, width), jnp.float32),
            pltpu.SemaphoreType.DMA((3 + chips // 2,)),
        ],
        compiler_params=pltpu.CompilerParams(vmem_limit_bytes=8 * 2**20),
    )(*results)


def on_device(saved_input, queries, keys, value_weight, grad_attended):
    token_count = queries.shape[0]
    local_width = value_weight.shape[1]
    local_heads = local_width // HD
    score_scale = 1.0 / jnp.sqrt(jnp.float32(HD))
    full_input = lax.all_gather(saved_input, "tensor", axis=1, tiled=True)
    values = jnp.dot(full_input, value_weight, preferred_element_type=jnp.float32).astype(
        jnp.bfloat16
    )
    query_heads = queries.reshape(token_count, local_heads, HD)
    key_heads = keys.reshape(token_count, local_heads, HD)
    value_heads = values.reshape(token_count, local_heads, HD)
    grad_heads = grad_attended.reshape(token_count, local_heads, HD)
    scores = (
        jnp.einsum("qhd,khd->hqk", query_heads, key_heads, preferred_element_type=jnp.float32)
        * score_scale
    )
    positions = lax.iota(jnp.int32, token_count)
    causal = positions[:, None] >= positions[None, :]
    scores = jnp.where(causal[None], scores, -jnp.inf)
    row_max = jnp.max(scores, axis=-1, keepdims=True)
    weights_exp = jnp.exp(scores - row_max)
    attention = weights_exp / jnp.sum(weights_exp, axis=-1, keepdims=True)
    probs_half = attention.astype(jnp.bfloat16)
    grad_values = jnp.einsum(
        "hqk,qhd->khd", probs_half, grad_heads, preferred_element_type=jnp.float32
    ).astype(jnp.bfloat16)
    grad_probs = jnp.einsum(
        "qhd,khd->hqk", grad_heads, value_heads, preferred_element_type=jnp.float32
    )
    row_dot = jnp.sum(attention * grad_probs, axis=-1, keepdims=True)
    grad_scores = (attention * (grad_probs - row_dot) * score_scale).astype(jnp.bfloat16)
    grad_queries = jnp.einsum(
        "hqk,khd->qhd", grad_scores, key_heads, preferred_element_type=jnp.float32
    ).astype(jnp.bfloat16)
    grad_keys = jnp.einsum(
        "hqk,qhd->khd", grad_scores, query_heads, preferred_element_type=jnp.float32
    ).astype(jnp.bfloat16)
    value_flat = grad_values.reshape(token_count, local_width)
    data_groups = lax.axis_size("dp")
    partial_value = lax.dot_general(
        value_flat, value_weight, (((1,), (1,)), ((), ())), preferred_element_type=jnp.float32
    )
    grad_input = lax.psum_scatter(
        partial_value.astype(jnp.bfloat16), "tensor", scatter_dimension=1, tiled=True
    )
    partial_value = lax.dot_general(
        full_input, value_flat, (((0,), (0,)), ((), ())), preferred_element_type=jnp.float32
    )
    summed = lax.psum_scatter(
        partial_value.astype(jnp.bfloat16), "dp", scatter_dimension=0, tiled=True
    ).astype(jnp.float32)
    grad_value_weight = summed / jnp.float32(data_groups)
    return (
        grad_input,
        grad_value_weight,
        grad_queries.reshape(token_count, local_width),
        grad_keys.reshape(token_count, local_width),
    )


def solution(mesh):
    placed = (
        P("dp", "tensor"),
        P("dp", "tensor"),
        P("dp", "tensor"),
        P(None, "tensor"),
        P("dp", "tensor"),
    )
    levels, groups = mesh.shape["tensor"], mesh.shape["dp"]
    run = on_device
    if groups == 2 * levels and levels == 4:
        run = functools.partial(fused, levels, groups)
    return jax.shard_map(
        run,
        mesh=mesh,
        in_specs=placed,
        out_specs=(P("dp", "tensor"), P("dp", "tensor"), P("dp", "tensor"), P("dp", "tensor")),
        check_vma=False,
    )
```
